32 devices in a mesh: rep: 2 (over x), dp: 16 (over y, z, core).
Axes of the slice: x: 2, y: 2, z: 4, core: 2. Of those that a mesh axis runs over, the one named last changes fastest.
Arguments:
- x: bfloat16 [32, 2048, 1024], P(('rep', 'dp')), parts along dimension 0
- dy: bfloat16 [32, 2048, 1024], P(('rep', 'dp')), parts along dimension 0
- w_gate: bfloat16 [2, 1024, 3200], replicated
- w_up: bfloat16 [2, 1024, 3200], replicated
- w_down: bfloat16 [2, 3200, 1024], replicated
- m_w_gate: float32 [2, 1024, 3200], P(None, 'dp')
- m_w_up: float32 [2, 1024, 3200], P(None, 'dp')
- m_w_down: float32 [2, 3200, 1024], P(None, 'dp')
- v_w_gate: float32 [2, 1024, 3200], P(None, 'dp')
- v_w_up: float32 [2, 1024, 3200], P(None, 'dp')
- v_w_down: float32 [2, 3200, 1024], P(None, 'dp')
Outputs:
- output 1: bfloat16 [4, 1024, 3200], P('rep'), parts along dimension 0
- output 2: bfloat16 [4, 1024, 3200], P('rep'), parts along dimension 0
- output 3: bfloat16 [4, 3200, 1024], P('rep'), parts along dimension 0
- output 4: float32 [4, 1024, 3200], P('rep', 'dp'), parts along dimension 0
- output 5: float32 [4, 1024, 3200], P('rep', 'dp'), parts along dimension 0
- output 6: float32 [4, 3200, 1024], P('rep', 'dp'), parts along dimension 0
- output 7: float32 [4, 1024, 3200], P('rep', 'dp'), parts along dimension 0
- output 8: float32 [4, 1024, 3200], P('rep', 'dp'), parts along dimension 0
- output 9: float32 [4, 3200, 1024], P('rep', 'dp'), parts along dimension 0
There are 2 independent parts. The reference program is written for one: setup_inputs(seed, part) draws one part's arguments, and reference() takes and returns one part's arrays. A program takes and returns all parts, laid end to end along the dimension named above; an argument that names none is the same for every part.
All inputs are finite; a program needn't handle non-finite values.
Results may differ from the reference program's by a relative error of at most 0.022.
Values are sent between devices in bfloat16 or wider.
A program may use at most 2 GiB of HBM per device.

```python
import jax
import jax.numpy as jnp
from jax import lax

SEQUENCES = 16
TOKENS = 2048
D = 1024
FF = 3200
LAYERS = 2
NAMES = ("w_gate", "w_up", "w_down")
SHAPES = {"w_gate": (LAYERS, D, FF), "w_up": (LAYERS, D, FF), "w_down": (LAYERS, FF, D)}


def bump(key, n, height):
    away = (jnp.arange(n, dtype=jnp.int32) - jax.random.randint(key, (), 0, n, jnp.int32)) % n
    return jnp.where(away < n // 8, height, 1.0)


def together(key, own, strength):
    shared = jax.random.normal(key, own.shape[1:], jnp.float32)
    return (own + strength * shared) * lax.rsqrt(1 + strength * strength)


def setup_inputs(seed: int = 0, part: int = 0) -> dict:
    kx, kdy, ka, kb, kz, kf, kh, kl, *keys = jax.random.split(jax.random.key(seed), 8 + 3 * len(NAMES))
    kx, kdy, ka, kb = (jax.random.fold_in(k, part) for k in (kx, kdy, ka, kb))
    kw, km, kv = (keys[i::3] for i in range(3))
    shape = (SEQUENCES, TOKENS, D)
    much_x, much_dy = jax.random.uniform(kz, (2,), jnp.float32, 0.0, 1.0)
    loud = 2.0 ** jax.random.uniform(jax.random.fold_in(kz, 1), (), jnp.float32, -1.0, 2.0)
    layers = 2.0 ** jax.random.uniform(kl, (LAYERS, 1, 1), jnp.float32, -1.0, 1.0)
    x = together(ka, jax.random.normal(kx, shape, jnp.float32), much_x) * bump(kf, D, 4.0)
    dy = together(kb, jax.random.normal(kdy, shape, jnp.float32), much_dy)
    drawn = {"x": x.astype(jnp.bfloat16), "dy": (loud * dy * (SEQUENCES * TOKENS) ** -0.5).astype(jnp.bfloat16)}
    for key, name in zip(kw, NAMES, strict=True):
        w = jax.random.normal(key, SHAPES[name], jnp.float32) * SHAPES[name][1] ** -0.5
        drawn[name] = (w * {"w_gate": 1.0, "w_up": bump(kh, FF, 4.0), "w_down": layers}[name]).astype(jnp.bfloat16)
    for key, name in zip(km, NAMES, strict=True):
        drawn[f"m_{name}"] = 0.1 * jax.random.normal(key, SHAPES[name], jnp.float32)
    for key, name in zip(kv, NAMES, strict=True):
        drawn[f"v_{name}"] = jax.random.uniform(key, SHAPES[name], jnp.float32, 0.005, 0.015)
    return drawn


def matmul(a, w):
    return jnp.dot(a, w, preferred_element_type=jnp.float32).astype(jnp.bfloat16)


def normed(h):
    wide = h.astype(jnp.float32)
    scale = lax.rsqrt(jnp.mean(wide**2, -1, keepdims=True) + 1e-6)
    return (wide * scale).astype(jnp.bfloat16)


def layer(h, w):
    a = normed(h)
    gate = jnp.dot(a, w["w_gate"], preferred_element_type=jnp.float32)
    up = jnp.dot(a, w["w_up"], preferred_element_type=jnp.float32)
    return h + matmul((jax.nn.silu(gate) * up).astype(jnp.bfloat16), w["w_down"])


def adamw(w, m, v, g):
    m = 0.9 * m + 0.1 * g
    v = 0.95 * v + 0.05 * g * g
    step = m * lax.rsqrt(v + 1e-8) + 0.1 * w
    return (w - 0.02 * step).astype(jnp.bfloat16), m, v


def stack(weights, h):
    return lax.scan(lambda h, w: (layer(h, w), None), h, weights)[0]


def reference(x, dy, w_gate, w_up, w_down, m_w_gate, m_w_up, m_w_down, v_w_gate, v_w_up, v_w_down):
    weights = dict(zip(NAMES, (w_gate, w_up, w_down), strict=True))

    def take(so_far, sequence):
        h, by_y = sequence
        _, back = jax.vjp(lambda w: stack(w, h), weights)
        return jax.tree.map(lambda total, term: total + term.astype(jnp.float32), so_far, back(by_y)[0]), None

    none_yet = {name: jnp.zeros(w.shape, jnp.float32) for name, w in weights.items()}
    by_weights, _ = lax.scan(take, none_yet, (x, dy))
    gradients = [by_weights[name].astype(jnp.bfloat16).astype(jnp.float32) for name in NAMES]
    new = [
        adamw(w.astype(jnp.float32), m, v, g)
        for w, m, v, g in zip((w_gate, w_up, w_down), (m_w_gate, m_w_up, m_w_down), (v_w_gate, v_w_up, v_w_down), gradients, strict=True)
    ]
    return tuple(one[which] for which in range(3) for one in new)
```

```python
import functools

import jax
import jax.numpy as jnp
from jax import lax
from jax.experimental import pallas as pl
from jax.experimental.pallas import tpu as pltpu
from jax.sharding import PartitionSpec as P

BF = jnp.bfloat16
F32 = jnp.float32
MESH = pl.DeviceIdType.MESH
NS = 8
NL = 4
LAST = 13


def _pieces(mat, a):
    if mat < 2:
        r = 64 // a
        return [(0, i * r, r, 0, i) for i in range(3)] + [(1, i * r, r, 0, 3 + i) for i in range(2)]
    t = 8 // a
    return [(0, i * 24, 24, 0, i) for i in range(t)] + [(1, i * 16, 16, 24, i) for i in range(t)]


def _dims(mat, a):
    return (64 // a, 640) if mat < 2 else (40, 1024 // a)


def _place(mat, a, s):
    if mat < 2:
        return (s % a) * (64 // a), pl.multiple_of((s // a) * 640, 128)
    return pl.multiple_of((s // a) * 40, 8), pl.multiple_of((s % a) * (1024 // a), 128)


def _cut(mat, a, s, part=None):
    r0, c0 = _place(mat, a, s)
    r, c = _dims(mat, a)
    if part is None:
        return pl.ds(r0, r), pl.ds(c0, c)
    if mat < 2:
        return pl.ds(r0, r), pl.ds(c0 + 384 * part, 256 if part else 384)
    return pl.ds(r0 + 24 * part, 16 if part else 24), pl.ds(c0, c)


def comm_kernel(a, *refs):
    g = (refs[0:3], refs[3:6])
    w, m, v = refs[6:9], refs[9:12], refs[12:15]
    ow, om, ov = refs[15:18], refs[18:21], refs[21:24]
    (own, oth, ry, ryz, rr, ll, mbuf, vbuf, wbuf,
     s_own, s_e, r_e, s_y, r_y, s_zr, r_zr, s_zl, r_zl, s_yz, r_yz, s_ld, s_st,
     s_ar, r_ar, s_al, r_al, s_ay, r_ay, s_br, r_br, s_bl, r_bl, s_by, r_by, s_c, r_c) = _group(refs[24:])
    per = 5 * a
    n = 6 * per
    rep, dp = lax.axis_index("rep"), lax.axis_index("dp")
    c, z, y = dp % 2, (dp // 2) % 4, dp // 8
    yz = y * 4 + z
    core, across, right, left = dp + 1 - 2 * c, dp + 8 - 16 * y, dp + 2, dp - 2

    def far(src, dst, ss, rs, to):
        return pltpu.make_async_remote_copy(src_ref=src, dst_ref=dst, send_sem=ss, recv_sem=rs, device_id=(rep, to), device_id_type=MESH)

    def near(src, dst, sem):
        return pltpu.make_async_copy(src, dst, sem)

    @pl.when(z == 0)
    def _():
        for p in range(2):
            rr[p][...] = jnp.zeros_like(rr[p])

    @pl.when(z == 3)
    def _():
        for p in range(2):
            ll[p][...] = jnp.zeros_like(ll[p])

    barrier = pltpu.get_barrier_semaphore()

    def greet(to):
        pl.semaphore_signal(barrier, inc=1, device_id=(rep, to), device_id_type=MESH)

    greet(core)
    greet(across)
    pl.when(z < 3)(lambda: greet(right))
    pl.when(z > 0)(lambda: greet(left))
    pl.semaphore_wait(barrier, 2 + jnp.where(z < 3, 1, 0) + jnp.where(z > 0, 1, 0))

    def what(k):
        mi = k // per
        return 1 - mi // 3, mi % 3, k % per

    def each(mat, do):
        def one(i):
            do(i)

        for i in range(3):
            pl.when(mat == i)(functools.partial(one, i))

    def stage(slot, st, do):
        k = slot - st
        pl.when((k >= 0) & (k < n))(lambda: do(k, k % NS))

    def fetch(k, q):
        layer, mat, s = what(k)

        def of(i, l):
            r0, c0 = _place(i, a, s)
            for part, d0, rows, s0, col in _pieces(i, a):
                at = (pl.ds(r0 + s0, rows), pl.ds(c0 + col * 128, 128))
                to = (q, slice(None), slice(None), pl.ds(d0, rows))
                near(g[l][i].at[(slice(None), slice(None), c, *at)], own[part].at[to], s_own.at[q, part]).start()
                far(g[l][i].at[(slice(None), slice(None), 1 - c, *at)], oth[part].at[to], s_e.at[q, part], r_e.at[q, part], core).start()

        for l in range(2):
            for i in range(3):
                pl.when((layer == l) & (mat == i))(functools.partial(of, i, l))

    def exchange(q, part):
        return far(own[part].at[q], oth[part].at[q], s_e.at[q, part], r_e.at[q, part], core)

    def f(x):
        return x.astype(F32)

    def y_send(q):
        return far(own[0].at[q, 1 - y], ry.at[q], s_y.at[q], r_y.at[q], across)

    def first(k, q):
        for part in range(2):
            near(own[part].at[q], own[part].at[q], s_own.at[q, part]).wait()
            exchange(q, part).wait_recv()

        def add(d):
            own[0][q, 1 - y, d] = (f(own[0][q, 1 - y, d]) + f(oth[0][q, 1 - y, d])).astype(BF)

        loop(0, 4, add)
        y_send(q).start()

    def line(part, q, d, to_right):
        ss, rs, buf = (s_zr, r_zr, rr) if to_right else (s_zl, r_zl, ll)
        to = right if to_right else left
        if part == 0:
            return far(own[0].at[q, y, d], buf[0].at[q, d], ss.at[part, q, d], rs.at[part, q, d], to)
        return far(own[1].at[q, :, d], buf[1].at[q, d], ss.at[part, q, d], rs.at[part, q, d], to)

    def total(part, q, d, buf):
        if part == 0:
            own[0][q, y, d] = (f(own[0][q, y, d]) + f(oth[0][q, y, d]) + f(ry[q, d]) + f(buf[0][q, d])).astype(BF)
        else:
            for j in range(2):
                own[1][q, j, d] = (f(own[1][q, j, d]) + f(oth[1][q, j, d]) + f(buf[1][q, d, j])).astype(BF)

    def loop(lo, hi, do):
        def one(d, _):
            do(d)
            return 0

        lax.fori_loop(lo, hi, one, 0)

    def go(to_right, part, k, q):
        buf = rr if to_right else ll

        def give(d):
            total(part, q, d, buf)
            line(part, q, d, to_right).start()

        def take(d):
            line(part, q, d, to_right).wait_recv()

        if to_right:
            pl.when(z > 0)(lambda: loop(z, 4, take))
            loop(z + 1, 4, give)
        else:
            pl.when(z < 3)(lambda: loop(0, z + 1, take))
            loop(0, z, give)

    def yz_send(q):
        return far(own[1].at[q, 1 - y, z], ryz.at[q], s_yz.at[q], r_yz.at[q], across)

    def yz(k, q):
        own[1][q, 1 - y, z] = (f(own[1][q, 1 - y, z]) + f(oth[1][q, 1 - y, z]) + f(rr[1][q, z, 1 - y]) + f(ll[1][q, z, 1 - y])).astype(BF)
        yz_send(q).start()

    def small(i, q, k, put):
        return [near(*d) for d in _small(i, q, k, put)]

    def _small(i, q, k, put):
        layer, _, s = what(k)
        rows, cols = _cut(i, a, s)
        x = k % NL
        t = 0 if i < 2 else 1
        if put:
            return [(mbuf[t].at[x], om[i].at[layer, rows, cols], s_st.at[x, 0]),
                    (vbuf[t].at[x], ov[i].at[layer, rows, cols], s_st.at[x, 1]),
                    (wbuf[t].at[x], ow[i].at[layer, y, z, c, rows, cols], s_st.at[x, 2])]
        return [(m[i].at[layer, rows, cols], mbuf[t].at[x], s_ld.at[x, 0]),
                (v[i].at[layer, rows, cols], vbuf[t].at[x], s_ld.at[x, 1]),
                (w[i].at[layer, y, z, c, rows, cols], wbuf[t].at[x], s_ld.at[x, 2])]

    def load(k, q):
        each(what(k)[1], lambda i: [d.start() for d in small(i, q, k, False)])

    def final(k, q):
        yz_send(q).wait_recv()
        x = k % NL

        def of(i):
            for d in small(i, q, k, False):
                d.wait()
            t = 0 if i < 2 else 1
            for part, d0, rows, s0, col in _pieces(i, a):
                at = pl.ds(d0, rows)
                if part == 0:
                    gr = (f(own[0][q, y, z, at]) + f(oth[0][q, y, z, at]) + f(ry[q, z, at])
                          + f(rr[0][q, z, at]) + f(ll[0][q, z, at]))
                else:
                    gr = (f(own[1][q, y, z, at]) + f(oth[1][q, y, z, at]) + f(rr[1][q, z, y, at])
                          + f(ll[1][q, z, y, at]) + f(ryz[q, at]))
                gr = f(gr.astype(BF))
                b = (x, pl.ds(s0, rows), pl.ds(col * 128, 128))
                mm = 0.9 * mbuf[t][b] + 0.1 * gr
                vv = 0.95 * vbuf[t][b] + 0.05 * gr * gr
                ww = f(wbuf[t][b])
                mbuf[t][b] = mm
                vbuf[t][b] = vv
                wbuf[t][b] = (ww - 0.02 * (mm * lax.rsqrt(vv + 1e-8) + 0.1 * ww)).astype(BF)
            for d in small(i, q, k, True):
                d.start()

        each(what(k)[1], of)

    def block(i, k, part, by, bz):
        layer, _, s = what(k)
        rows, cols = _cut(i, a, s, part)
        return ow[i].at[layer, by, bz, c, rows, cols]

    def pair(i, k, bz):
        layer, _, s = what(k)
        rows, cols = _cut(i, a, s, 1)
        return ow[i].at[layer, :, bz, c, rows, cols]

    def same(ref, ss, rs, to):
        return lambda: far(ref, ref, ss, rs, to)

    def moves(i, k, q, t):
        out = []
        b = block(i, k, 0, y, z)
        cs = s_c.at
        if t == 0:
            out.append((None, None, [
                (z < 3, same(b, s_ar.at[q, 0], r_ar.at[q, 0], right)),
                (z > 0, same(b, s_al.at[q, 0], r_al.at[q, 0], left)),
                (None, same(b, s_ay.at[q, 0], r_ay.at[q, 0], across)),
                (None, same(b, cs[q, 0], r_c.at[k % (2 * NS)], core)),
            ]))
            e = block(i, k, 1, y, z)
            out.append((None, None, [
                (None, same(e, s_by.at[q], r_by.at[q], across)),
                (None, same(e, cs[q, 14], r_c.at[k % (2 * NS)], core)),
            ]))
        if 1 <= t <= 3:
            b = block(i, k, 0, y, z - t)
            sends = [(None, same(b, s_ay.at[q, t], r_ay.at[q, t], across)), (None, same(b, cs[q, t], r_c.at[k % (2 * NS)], core))]
            if t < 3:
                sends.insert(0, (z < 3, same(b, s_ar.at[q, t], r_ar.at[q, t], right)))
            out.append((z >= t, same(b, s_ar.at[q, t - 1], r_ar.at[q, t - 1], right), sends))
            b = block(i, k, 0, y, z + t)
            sends = [(None, same(b, s_ay.at[q, 3 + t], r_ay.at[q, 3 + t], across)), (None, same(b, cs[q, 3 + t], r_c.at[k % (2 * NS)], core))]
            if t < 3:
                sends.insert(0, (z > 0, same(b, s_al.at[q, t], r_al.at[q, t], left)))
            out.append((z + t <= 3, same(b, s_al.at[q, t - 1], r_al.at[q, t - 1], left), sends))
        if 1 <= t <= 4:
            u = t - 1
            b = block(i, k, 0, 1 - y, z - u)
            out.append((None if u == 0 else z >= u, same(b, s_ay.at[q, u], r_ay.at[q, u], across), [(None, same(b, cs[q, 7 + u], r_c.at[k % (2 * NS)], core))]))
            if u:
                b = block(i, k, 0, 1 - y, z + u)
                out.append((z + u <= 3, same(b, s_ay.at[q, 3 + u], r_ay.at[q, 3 + u], across), [(None, same(b, cs[q, 10 + u], r_c.at[k % (2 * NS)], core))]))
        if t == 1:
            e, p = block(i, k, 1, 1 - y, z), pair(i, k, z)
            out.append((None, same(e, s_by.at[q], r_by.at[q], across), [
                (z < 3, same(p, s_br.at[q, 0], r_br.at[q, 0], right)),
                (z > 0, same(p, s_bl.at[q, 0], r_bl.at[q, 0], left)),
                (None, same(e, cs[q, 15], r_c.at[k % (2 * NS)], core)),
            ]))
        if 2 <= t <= 4:
            u = t - 1
            p = pair(i, k, z - u)
            sends = [(None, same(p, cs[q, 15 + u], r_c.at[k % (2 * NS)], core))]
            if u < 3:
                sends.insert(0, (z < 3, same(p, s_br.at[q, u], r_br.at[q, u], right)))
            out.append((z >= u, same(p, s_br.at[q, u - 1], r_br.at[q, u - 1], right), sends))
            p = pair(i, k, z + u)
            sends = [(None, same(p, cs[q, 18 + u], r_c.at[k % (2 * NS)], core))]
            if u < 3:
                sends.insert(0, (z > 0, same(p, s_bl.at[q, u], r_bl.at[q, u], left)))
            out.append((z + u <= 3, same(p, s_bl.at[q, u - 1], r_bl.at[q, u - 1], left), sends))
        return out

    def when(cond, do):
        do() if cond is None else pl.when(cond)(lambda: do())

    def spread(t, k, q):
        def of(i):
            if t == 0:
                for d in small(i, q, k, True):
                    d.wait()
            for cond, wait, sends in moves(i, k, q, t):
                def go(wait=wait, sends=sends):
                    if wait is not None:
                        wait().wait_recv()
                    for on, copy in sends:
                        when(on, lambda copy=copy: copy().start())
                when(cond, go)

        each(what(k)[1], of)

    def finish(k, q):
        def of(i):
            layer, _, s = what(k)
            rows, cols = _cut(i, a, s)
            b = ow[i].at[layer, :, :, 1 - c, rows, cols]
            same(b, s_c.at[q, 0], r_c.at[k % (2 * NS)], core)().wait_recv()
            for t in range(5):
                for cond, _, sends in moves(i, k, q, t):
                    def go(sends=sends):
                        for on, copy in sends:
                            when(on, lambda copy=copy: copy().wait_send())
                    when(cond, go)

        each(what(k)[1], of)

    def sent(k, q):
        for part in range(2):
            exchange(q, part).wait_send()

            loop(z + 1, 4, lambda d, part=part: line(part, q, d, True).wait_send())
            loop(0, z, lambda d, part=part: line(part, q, d, False).wait_send())
        y_send(q).wait_send()
        yz_send(q).wait_send()

    def slot(i, _):
        stage(i, 0, fetch)
        stage(i, 1, first)
        stage(i, 2, lambda k, q: y_send(q).wait_recv())
        for part, base in ((1, 1), (0, 2)):
            stage(i, base + z, functools.partial(go, True, part))
            stage(i, base + 3 - z, functools.partial(go, False, part))
        stage(i, 4, yz)
        stage(i, 3, load)
        stage(i, 5, final)
        for t in range(5):
            stage(i, 6 + t, functools.partial(spread, t))
        stage(i, 7, sent)
        stage(i, 12, finish)
        return 0

    lax.fori_loop(0, n + LAST, slot, 0)


def _scratch(a):
    ry, rz = 192 // a, 128 // a
    d = pltpu.SemaphoreType.DMA
    A, B = _dims(0, a), _dims(2, a)
    shapes = [
        [pltpu.VMEM((NS, 2, 4, r, 128), BF) for r in (ry, rz)],
        [pltpu.VMEM((NS, 2, 4, r, 128), BF) for r in (ry, rz)],
        pltpu.VMEM((NS, 4, ry, 128), BF),
        pltpu.VMEM((NS, rz, 128), BF),
        [pltpu.VMEM((NS, 4, ry, 128), BF), pltpu.VMEM((NS, 4, 2, rz, 128), BF)],
        [pltpu.VMEM((NS, 4, ry, 128), BF), pltpu.VMEM((NS, 4, 2, rz, 128), BF)],
        [pltpu.VMEM((NL, *A), F32), pltpu.VMEM((NL, *B), F32)],
        [pltpu.VMEM((NL, *A), F32), pltpu.VMEM((NL, *B), F32)],
        [pltpu.VMEM((NL, *A), BF), pltpu.VMEM((NL, *B), BF)],
        d((NS, 2)), d((NS, 2)), d((NS, 2)), d((NS,)), d((NS,)),
        d((2, NS, 4)), d((2, NS, 4)), d((2, NS, 4)), d((2, NS, 4)), d((NS,)), d((NS,)), d((NL, 3)), d((NL, 3)),
        d((NS, 3)), d((NS, 3)), d((NS, 3)), d((NS, 3)), d((NS, 7)), d((NS, 7)),
        d((NS, 3)), d((NS, 3)), d((NS, 3)), d((NS, 3)), d((NS,)), d((NS,)), d((NS, 22)), d((2 * NS,)),
    ]
    return shapes


def _group(flat):
    like, out, j = _scratch(1), [], 0
    for s in like:
        if isinstance(s, list):
            out.append(flat[j : j + len(s)])
            j += len(s)
        else:
            out.append(flat[j])
            j += 1
    return out


def comm(g0, g1, w, m, v, a=1):
    def blocks(t):
        lead = t.shape[:-2]
        return t.reshape(*lead, 2, 4, 2, t.shape[-2] // 16, t.shape[-1])

    args = [blocks(t) for t in (*g0, *g1, *w)] + [*m, *v]
    outs = [jax.ShapeDtypeStruct(blocks(t).shape, BF) for t in w] + [jax.ShapeDtypeStruct(t.shape, F32) for t in (*m, *v)]
    flat = [x for s in _scratch(a) for x in (s if isinstance(s, list) else [s])]
    new = pl.pallas_call(
        functools.partial(comm_kernel, a),
        out_shape=outs,
        in_specs=[pl.BlockSpec(memory_space=pl.ANY)] * len(args),
        out_specs=[pl.BlockSpec(memory_space=pl.ANY)] * len(outs),
        scratch_shapes=flat,
        compiler_params=pltpu.CompilerParams(collective_id=0, has_side_effects=True, vmem_limit_bytes=60 << 20),
    )(*args)
    return [n.reshape(t.shape) for n, t in zip(new, (*w, *m, *v))]


def dot(a, b, dims, out=F32):
    return lax.dot_general(a, b, (dims, ((), ())), preferred_element_type=F32).astype(out)


def normed(h):
    wide = h.astype(F32)
    scale = lax.rsqrt(jnp.mean(wide**2, -1, keepdims=True) + 1e-6)
    return (wide * scale).astype(BF), scale


def normed_back(h, scale, da):
    wide, da = h.astype(F32), da.astype(F32)
    inner = jnp.mean(wide * da, -1, keepdims=True)
    return (scale * da - wide * (scale * scale * scale * inner)).astype(BF)


def gated(gate, up):
    return (gate * jax.nn.sigmoid(gate) * up).astype(BF)


def gated_back(gate, up, dhid):
    s = jax.nn.sigmoid(gate)
    dhid = dhid.astype(F32)
    dup = dhid * gate * s
    dgate = dhid * up * (s + gate * s * (1 - s))
    return dgate.astype(BF), dup.astype(BF)


def gradients(x, dy, wg, wu, wd):
    a0, s0 = normed(x)
    gate0 = dot(a0, wg[0], ((1,), (0,)))
    up0 = dot(a0, wu[0], ((1,), (0,)))
    hid0 = gated(gate0, up0)
    h1 = x + dot(hid0, wd[0], ((1,), (0,)), BF)
    a1, s1 = normed(h1)
    gate1 = dot(a1, wg[1], ((1,), (0,)))
    up1 = dot(a1, wu[1], ((1,), (0,)))
    hid1 = gated(gate1, up1)
    out = []

    def back(a, gate, up, hid, dout, wg, wu, wd):
        dhid = dot(dout, wd, ((1,), (1,)), BF)
        dwd = dot(hid, dout, ((0,), (0,)), BF)
        dgate, dup = gated_back(gate, up, dhid)
        dwg = dot(a, dgate, ((0,), (0,)), BF)
        dwu = dot(a, dup, ((0,), (0,)), BF)
        return dgate, dup, dwg, dwu, dwd

    dgate, dup, *g1 = back(a1, gate1, up1, hid1, dy, wg[1], wu[1], wd[1])
    da = dot(dgate, wg[1], ((1,), (1,)), BF) + dot(dup, wu[1], ((1,), (1,)), BF)
    dh1 = dy + normed_back(h1, s1, da)
    _, _, *g0 = back(a0, gate0, up0, hid0, dh1, wg[0], wu[0], wd[0])
    return g1, g0


def solution(mesh):
    def step(x, dy, *arrays):
        w, m, v = (arrays[i : i + 3] for i in (0, 3, 6))
        g1, g0 = gradients(x[0], dy[0], *w)
        return tuple(comm(g0, g1, w, m, v, 2))

    one, whole, rows = P(("rep", "dp")), P(), P(None, "dp")
    return jax.shard_map(
        step,
        mesh=mesh,
        in_specs=(one, one) + (whole,) * 3 + (rows,) * 6,
        out_specs=(P("rep"),) * 3 + (P("rep", "dp"),) * 6,
        check_vma=False,
    )
```

```python
import functools

import jax
import jax.numpy as jnp
from jax import lax
from jax.experimental import pallas as pl
from jax.experimental.pallas import tpu as pltpu
from jax.sharding import PartitionSpec as P

BF, F32 = jnp.bfloat16, jnp.float32
MESH = pl.DeviceIdType.MESH
ALL = slice(None)
T, D, F, FB, LANES = 2048, 1024, 3200, 640, 128
BLOCKS = F // FB
TT, TILES = 512, 4
HALF = T // 2
LINE = 4
NS = 8
NL, NW = 4, 16
LAST = 11
LEAD = 3
GATE, UP, DOWN = range(3)
SHAPE = {GATE: (32, FB), UP: (32, FB), DOWN: (40, 512)}
FIRST = {GATE: (32, 384), UP: (32, 384), DOWN: (24, 512)}
MANY = 2
ROWS = (96, 64)
NGU, ND = 20, 10
N = 2 * (NGU + ND)
DA, LOW = 4 * BLOCKS, 4 * BLOCKS + 2 * BLOCKS
END = LOW + 4 * BLOCKS


def _dot(p, q, cp, cq):
    return lax.dot_general(p, q, (((cp,), (cq,)), ((), ())), preferred_element_type=F32)


def f(x):
    return x.astype(F32)


def near(src, dst, sem):
    return pltpu.make_async_copy(src, dst, sem)


def at(k, size):
    return pl.ds(pl.multiple_of(k * size, size), size)


def loop(lo, hi, do):
    def one(d, _):
        do(d)
        return 0

    lax.fori_loop(lo, hi, one, 0)


def run(copies):
    for c in copies:
        c.start()


def wait(copies):
    for c in copies:
        c.wait()


def pieces(kind):
    (r, c), (r0, c0) = SHAPE[kind], FIRST[kind]
    if kind < DOWN:
        left = c0 // LANES
        return [(0, i * r, r, 0, i) for i in range(left)] + [(1, (i - left) * r, r, 0, i) for i in range(left, c // LANES)]
    return [(p, i * k, k, o, i) for p, k, o in ((0, r0, 0), (1, r - r0, r0)) for i in range(c // LANES)]


def cut(kind, s, part=None):
    (r, c), (r0, c0) = SHAPE[kind], FIRST[kind]
    row, col = (s % MANY, s // MANY) if kind < DOWN else (s // MANY, s % MANY)
    row, col = pl.multiple_of(row * r, 8), pl.multiple_of(col * c, LANES)
    if part is None:
        return pl.ds(row, r), pl.ds(col, c)
    if kind < DOWN:
        return pl.ds(row, r), pl.ds(col + c0, c - c0) if part else pl.ds(col, c0)
    return pl.ds(row + r0, r - r0) if part else pl.ds(row, r0), pl.ds(col, c)


def step_kernel(*refs):
    refs = list(refs)

    def take(n):
        out = refs[:n]
        del refs[:n]
        return out

    x, dy = take(2)
    nat, w, m, v, ow, om, ov, g = (take(3) for _ in range(8))
    dgu_all, gate0, up0, a0, h1 = take(5)
    own, oth, rr, ll, mbuf, vbuf, wbuf = (take(2) for _ in range(7))
    (ry, ryz, s_own, s_e, r_e, s_y, r_y, s_zr, r_zr, s_zl, r_zl, s_yz, r_yz, s_ld, s_st,
     s_ar, r_ar, s_al, r_al, s_ay, r_ay, s_br, r_br, s_bl, r_bl, s_by, r_by, s_c, r_c,
     av, dv, wgu, wd, hid, dgu, gout, dout, acc, gt,
     s_x, s_dy, s_w, s_wd, s_dgu, s_go, s_do, s_dl, s_gt, s_h, s_a0, s_keep, s_h1) = refs
    rep, dp = lax.axis_index("rep"), lax.axis_index("dp")
    c, z, y = dp % 2, (dp // 2) % LINE, dp // (2 * LINE)
    core, across, right, left = dp + 1 - 2 * c, dp + (1 - 2 * y) * 2 * LINE, dp + 2, dp - 2
    more, less = z < LINE - 1, z > 0

    def far(src, dst, ss, rs, to):
        return pltpu.make_async_remote_copy(src_ref=src, dst_ref=dst, send_sem=ss, recv_sem=rs, device_id=(rep, to), device_id_type=MESH)

    def clear(bufs):
        for b in bufs:
            b[...] = jnp.zeros_like(b)

    pl.when(z == 0)(lambda: clear(rr))
    pl.when(z == LINE - 1)(lambda: clear(ll))
    barrier = pltpu.get_barrier_semaphore()

    def greet(to):
        pl.semaphore_signal(barrier, inc=1, device_id=(rep, to), device_id_type=MESH)

    greet(core)
    greet(across)
    pl.when(more)(lambda: greet(right))
    pl.when(less)(lambda: greet(left))
    def what(k):
        u = k % (NGU + ND)
        gu = u < NGU
        return 1 - k // (NGU + ND), jnp.where(gu, (u // 2) % 2, DOWN), jnp.where(gu, (u // 4) * 2 + u % 2, u - NGU)

    def each(kind, do):
        def one(i):
            do(i)

        for i in SHAPE:
            pl.when(kind == i)(functools.partial(one, i))

    def stage(tick, st, do):
        k = tick - st
        pl.when((k >= 0) & (k < N))(lambda: do(k, k % NS))

    def fetch(k, q):
        layer, kind, s = what(k)

        def of(i):
            rows, cols = cut(i, s)
            for part, d0, n, s0, col in pieces(i):
                cc = pl.ds(cols.start + col * LANES, LANES)
                here = (pl.ds(rows.start + s0, n), cc) if i < DOWN else (s // MANY, pl.ds(s0, n), cc)
                to = (q, ALL, ALL, pl.ds(d0, n))
                mine, other = ((layer, ALL, ALL, h, *here) for h in (c, 1 - c))
                src = g[i]
                near(src.at[mine], own[part].at[to], s_own.at[q, part]).start()
                far(src.at[other], oth[part].at[to], s_e.at[q, part], r_e.at[q, part], core).start()

        each(kind, of)

    def exchange(q, part):
        return far(own[part].at[q], oth[part].at[q], s_e.at[q, part], r_e.at[q, part], core)

    def y_send(q):
        return far(own[0].at[q, 1 - y], ry.at[q], s_y.at[q], r_y.at[q], across)

    def first(k, q):
        for part in range(2):
            near(own[part].at[q], own[part].at[q], s_own.at[q, part]).wait()
            exchange(q, part).wait_recv()

        def add(d):
            own[0][q, 1 - y, d] = (f(own[0][q, 1 - y, d]) + f(oth[0][q, 1 - y, d])).astype(BF)

        loop(0, LINE, add)
        y_send(q).start()

    def line(part, q, d, to_right):
        ss, rs, buf, to = (s_zr, r_zr, rr, right) if to_right else (s_zl, r_zl, ll, left)
        src = own[0].at[q, y, d] if part == 0 else own[1].at[q, :, d]
        return far(src, buf[part].at[q, d], ss.at[part, q, d], rs.at[part, q, d], to)

    def total(part, q, d, buf):
        if part == 0:
            own[0][q, y, d] = (f(own[0][q, y, d]) + f(oth[0][q, y, d]) + f(ry[q, d]) + f(buf[0][q, d])).astype(BF)
        else:
            for j in range(2):
                own[1][q, j, d] = (f(own[1][q, j, d]) + f(oth[1][q, j, d]) + f(buf[1][q, d, j])).astype(BF)

    def go(to_right, part, k, q):
        def get(d):
            line(part, q, d, to_right).wait_recv()

        def give(d):
            total(part, q, d, rr if to_right else ll)
            line(part, q, d, to_right).start()

        if to_right:
            pl.when(less)(lambda: loop(z, LINE, get))
            loop(z + 1, LINE, give)
        else:
            pl.when(more)(lambda: loop(0, z + 1, get))
            loop(0, z, give)

    def yz_send(q):
        return far(own[1].at[q, 1 - y, z], ryz.at[q], s_yz.at[q], r_yz.at[q], across)

    def yz(k, q):
        b, r = (q, 1 - y, z), (q, z, 1 - y)
        own[1][b] = (f(own[1][b]) + f(oth[1][b]) + f(rr[1][r]) + f(ll[1][r])).astype(BF)
        yz_send(q).start()

    def small(i, k, put):
        layer, _, s = what(k)
        rows, cols = cut(i, s)
        e, t = k % NL, i // DOWN
        block = (layer, y, z, c, rows, cols)
        there = ((om if put else m)[i].at[layer, rows, cols], (ov if put else v)[i].at[layer, rows, cols], (ow if put else w)[i].at[block])
        here = (mbuf[t].at[e], vbuf[t].at[e], wbuf[t].at[k % NW])
        sems = s_st if put else s_ld
        return [near(b, r, sems.at[e, h]) if put else near(r, b, sems.at[e, h]) for h, (r, b) in enumerate(zip(there, here, strict=True))]

    def final(k, q):
        yz_send(q).wait_recv()

        def of(i):
            wait(small(i, k, False))
            mb, vb, wb = (b[i // DOWN] for b in (mbuf, vbuf, wbuf))
            for part, d0, n, s0, col in pieces(i):
                r = pl.ds(d0, n)
                gr = f(own[part][q, y, z, r]) + f(oth[part][q, y, z, r])
                gr += f(ry[q, z, r]) + f(rr[0][q, z, r]) + f(ll[0][q, z, r]) if part == 0 else f(rr[1][q, z, y, r]) + f(ll[1][q, z, y, r]) + f(ryz[q, r])
                gr = f(gr.astype(BF))
                b = (pl.ds(s0, n), pl.ds(col * LANES, LANES))
                bm, bw = (k % NL, *b), (k % NW, *b)
                mm = 0.9 * mb[bm] + 0.1 * gr
                vv = 0.95 * vb[bm] + 0.05 * gr * gr
                ww = f(wb[bw])
                mb[bm] = mm
                vb[bm] = vv
                wb[bw] = (ww - 0.02 * (mm * lax.rsqrt(vv + 1e-8) + 0.1 * ww)).astype(BF)
            run(small(i, k, True))

        each(what(k)[1], of)
        spread(0, k, q)

    def moves(i, k, q, t):
        layer, _, s = what(k)
        dst = ow[i]

        def block(part, by, bz):
            return dst.at[(layer, by, bz, c, *cut(i, s, part))]

        def mine(part):
            r, cc = SHAPE[i][0] if i < DOWN else FIRST[i][0], FIRST[i][1]
            if part:
                r, cc = (pl.ds(0, r), pl.ds(cc, FB - cc)) if i < DOWN else (pl.ds(r, SHAPE[i][0] - r), pl.ds(0, cc))
            else:
                r, cc = pl.ds(0, r), pl.ds(0, cc)
            return wbuf[i // DOWN].at[k % NW, r, cc]

        def same(ref, ss, rs, n, to, src=None):
            n = q if n is None else (q, n)
            return lambda: far(ref if src is None else src, ref, ss.at[n], rs.at[n], to)

        def along(part, b, n, src=None):
            sr, gr, sl, gl_ = (s_ar, r_ar, s_al, r_al) if part == 0 else (s_br, r_br, s_bl, r_bl)
            return same(b, sr, gr, n, right, src), same(b, sl, gl_, n, left, src)

        out = []
        side = LINE - 1
        b, e = block(0, y, z), block(1, y, z)
        if t == 0:
            r, l = along(0, b, 0, mine(0))
            out.append((None, None, [(more, r), (less, l), (None, same(b, s_ay, r_ay, 0, across, mine(0))), (None, same(e, s_by, r_by, None, across, mine(1)))]))
        elif t <= side:
            for sign, on in ((-1, z >= t), (1, z + t <= side)):
                b = block(0, y, z + sign * t)
                to = 0 if sign < 0 else 1
                sends = [(None, same(b, s_ay, r_ay, t if sign < 0 else side + t, across))]
                if t < side:
                    sends.insert(0, ((more, less)[to], along(0, b, t)[to]))
                out.append((on, along(0, b, t - 1)[to], sends))
        u = t - 1
        if u >= 0:
            for sign, on in ((-1, z >= u), (1, z + u <= side))[: 1 if u == 0 else 2]:
                b = block(0, 1 - y, z + sign * u)
                out.append((on, same(b, s_ay, r_ay, u if sign < 0 else side + u, across), []))
        if u == 0:
            r, l = along(1, dst.at[(layer, ALL, z, c, *cut(i, s, 1))], 0)
            out.append((None, same(e, s_by, r_by, None, across), [(more, r), (less, l)]))
        elif u > 0:
            for sign, on in ((-1, z >= u), (1, z + u <= side)):
                b = dst.at[(layer, ALL, z + sign * u, c, *cut(i, s, 1))]
                to = 0 if sign < 0 else 1
                out.append((on, along(1, b, u - 1)[to], [((more, less)[to], along(1, b, u)[to])] if u < side else []))
        return out

    def when(cond, do):
        do() if cond is None else pl.when(cond)(lambda: do())

    def spread(t, k, q):
        def of(i):
            if t == 1:
                wait(small(i, k, True))
            for cond, first_, sends in moves(i, k, q, t):

                def act(first_=first_, sends=sends):
                    if first_ is not None:
                        first_().wait_recv()
                    for on, copy in sends:
                        when(on, lambda copy=copy: copy().start())

                when(cond, act)

        each(what(k)[1], of)

    def over(i, k, q):
        layer, _, s = what(k)
        b = ow[i].at[(layer, ALL, ALL, c, *cut(i, s))]
        return far(b, b, s_c.at[q], r_c.at[k % (2 * NS)], core)

    def hand(k, q):
        each(what(k)[1], lambda i: over(i, k, q).start())

    def finish(k, q):
        def of(i):
            over(i, k, q).wait()
            for t in range(LINE + 1):
                for cond, _, sends in moves(i, k, q, t):

                    def act(sends=sends):
                        for on, copy in sends:
                            when(on, lambda copy=copy: copy().wait_send())

                    if sends:
                        when(cond, act)

        each(what(k)[1], of)

    def sent(k, q):
        for part in range(2):
            exchange(q, part).wait_send()
            loop(z + 1, LINE, lambda d, part=part: line(part, q, d, True).wait_send())
            loop(0, z, lambda d, part=part: line(part, q, d, False).wait_send())
        y_send(q).wait_send()
        yz_send(q).wait_send()

    def communicate(i):
        stage(i, 0, first)
        stage(i, 1, lambda k, q: y_send(q).wait_recv())
        for part in (1, 0):
            base = 1 - part
            stage(i, base + z, functools.partial(go, True, part))
            stage(i, base + LINE - 1 - z, functools.partial(go, False, part))
        stage(i, LINE - 1, yz)
        stage(i, LINE - 2, lambda k, q: each(what(k)[1], lambda e: run(small(e, k, False))))
        stage(i, LINE, final)
        for t in range(1, LINE + 1):
            stage(i, LINE + t, functools.partial(spread, t))
        stage(i, 2 * LINE, hand)
        stage(i, NS - 2, sent)
        stage(i, LAST - 1, finish)

    def wload(layer, j, x):
        return [near(nat[h].at[layer, :, at(j, FB)], wgu.at[x, :, pl.ds(FB * h, FB)], s_w.at[x, h]) for h in range(2)]

    def wdload(layer, j, x):
        return near(nat[DOWN].at[layer, at(j, FB)], wd.at[x], s_wd.at[x])

    def x_tile(t):
        return near(x.at[at(t, TT)], dgu.at[at(t, TT), pl.ds(0, D)], s_x.at[t])

    def h1_tile(t):
        return near(dgu.at[at(t, TT), pl.ds(0, D)], h1.at[at(t, TT)], s_h1.at[t])

    def dy_tile(t):
        return near(dy.at[at(t, TT)], dv.at[at(t, TT)], s_dy.at[t])

    def a0_load():
        return near(a0, av, s_a0)

    def a0_keep():
        return near(av, a0, s_a0)

    def keep(j):
        return near(dgu, dgu_all.at[j], s_dgu)

    def dl(u):
        return near(dgu_all.at[u % BLOCKS, at(u // BLOCKS, HALF)], dgu.at[at(u % 2, HALF)], s_dl.at[u % 2])

    def gl(s, put=False):
        e = s % 3
        here = [(t.at[at(s % TILES, TT), at(s // TILES, FB)], gt.at[e, h]) for h, t in enumerate((gate0, up0))]
        return [near(b, t, s_keep.at[e, h]) if put else near(t, b, s_gt.at[e, h]) for h, (t, b) in enumerate(here)]

    def h1_load():
        return near(h1, av, s_h)

    def g_out(layer, j, t):
        return [near(gout.at[t, :, :, :, pl.ds(FB * h, FB)], g[h].at[layer, t, :, :, :, at(j, FB)], s_go.at[t, h]) for h in range(2)]

    def _rms(b):
        wide = f(b)
        return (wide * lax.rsqrt(jnp.mean(wide * wide, -1, keepdims=True) + 1e-6)).astype(BF)

    def down(s):
        rows, j = at(s % TILES, TT), s // TILES
        acc[rows] = jnp.where(j == 0, 0.0, acc[rows]) + _dot(hid[at(s % 2, TT)], wd[j % 2], 1, 0)

    def close(t):
        rows = at(t, TT)
        new = (f(dgu[rows, :D]) + f(acc[rows].astype(BF))).astype(BF)
        dgu[rows, :D] = new
        av[rows] = _rms(new)
        h1_tile(t).start()

    STEPS = BLOCKS * TILES

    def forward(s):
        j, t = s // TILES, s % TILES
        k = j % 2
        rows = at(t, TT)

        @pl.when(t == 0)
        def _():
            wait(wload(0, j, k))
            wdload(0, j, k).wait()

        @pl.when(t == 1)
        def _():
            last = j == BLOCKS - 1
            layer, nxt = jnp.where(last, 1, 0), jnp.where(last, 0, j + 1)
            run(wload(layer, nxt, 1 - k))
            wdload(layer, nxt, 1 - k).start()

        pl.when(s == TILES)(lambda: a0_keep().start())
        pl.when(s == STEPS - TILES)(lambda: a0_keep().wait())
        pl.when(s >= 3)(lambda: wait(gl(s - 3, True)))

        @pl.when(j == 0)
        def _():
            x_tile(t).wait()
            av[rows] = _rms(dgu[rows, :D])

        gu = _dot(av[rows], wgu[k], 1, 0)
        down(jnp.where(s == 0, TILES - 1, s - 1))
        gate, up = gu[:, :FB], gu[:, FB:]
        gt[s % 3, 0] = gate
        gt[s % 3, 1] = up
        hid[at(s % 2, TT)] = (gate * jax.nn.sigmoid(gate) * up).astype(BF)
        run(gl(s, True))
        pl.when(s > STEPS - TILES)(lambda: close(t - 1))

    def gated(rows, gate, up, dh):
        s = jax.nn.sigmoid(gate)
        gs = gate * s
        dh = f(dh.astype(BF))
        hid[rows] = (gs * up).astype(BF)
        dgu[rows, FB:] = (dh * gs).astype(BF)
        dgu[rows, :FB] = (dh * up * (s + gs * (1 - s))).astype(BF)

    def gu_half(t, layer, j):
        out = _dot(av[:, at(t, TT)], dgu[...], 0, 0).astype(BF)
        gout[t] = out.reshape(gout.shape[1:])
        run(g_out(layer, j, t))

    def where(i):
        top, low = i < DA, (i >= LOW) & (i < END)
        ii = jnp.where(top, i, i - LOW)
        return top, low, ii // 4, ii % 4, jnp.where(top, 1, 0)

    def before(i):
        top, low, j, r, layer = where(i)

        @pl.when((top | low) & (r == 3))
        def _():
            for t in range(2):
                wait(g_out(layer, j, t))

        stage(i, LEAD, fetch)

    def compute(i):
        top, low, j, r, layer = where(i)
        x = jnp.where(top, j + 1, j) % 2

        pl.when(((i > 4) & (i <= DA + 1) & (i % 4 == 1)) | ((i > LOW + 4) & (i <= END + 1) & (i % 4 == (LOW + 1) % 4)))(lambda: near(dout, dout, s_do).wait())

        @pl.when(top & (r == 0))
        def _():
            wait(wload(1, j, x))
            wdload(1, j, x).wait()
            pl.when(j > 0)(lambda: keep(j - 1).wait())

            @pl.when(j < BLOCKS - 1)
            def _():
                run(wload(1, j + 1, 1 - x))
                wdload(1, j + 1, 1 - x).start()

        @pl.when(top & (r < 2))
        def _():
            def one(t):
                pl.when(j == 0)(lambda: wait((dy_tile(t), h1_tile(t))))
                rows = at(t, TT)
                gu = _dot(av[rows], wgu[x], 1, 0)
                gated(rows, gu[:, :FB], gu[:, FB:], _dot(dv[rows], wd[x], 1, 1))

            loop(2 * r, 2 * r + 2, one)
            pl.when(r == 1)(lambda: keep(j).start())

        @pl.when(low & (r == 0))
        def _():
            wdload(0, j, x).wait()
            pl.when(j < BLOCKS - 1)(lambda: wdload(0, j + 1, 1 - x).start())

        @pl.when(low & (r < 2))
        def _():
            def one(t):
                s = TILES * j + t
                wait(gl(s))
                pl.when(s < BLOCKS * TILES - 2)(lambda: run(gl(s + 2)))
                rows = at(t, TT)
                gated(rows, gt[s % 3, 0], gt[s % 3, 1], _dot(dv[rows], wd[x], 1, 1))

            loop(3 * r, 3 + r, one)

        @pl.when((top & (r == 2)) | (low & ((r == 1) | (r == 2))))
        def _():
            pl.when(i == LOW + 1)(lambda: a0_load().wait())
            loop(jnp.where(top, 0, r - 1), jnp.where(top, 2, r), lambda t: gu_half(t, layer, j))

        @pl.when((top | low) & (r == 3))
        def _():
            out = _dot(hid[...], dv[...], 0, 0)
            pp, n = dout.shape[:2]
            for p in range(pp):
                dout[p] = out[n * p : n * (p + 1)].astype(BF)

            def send(p):
                o = pp * j + p
                near(dout.at[p], g[DOWN].at[layer, o // 40, (o // 10) % LINE, (o // 5) % 2, o % 5], s_do).start()

            loop(0, pp, send)

        @pl.when(i == DA - 1)
        def _():
            keep(BLOCKS - 1).wait()
            run(wload(1, 0, 0))
            dl(0).start()
            h1_load().start()

        @pl.when((i >= DA) & (i < LOW))
        def _():
            u = i - DA
            j, x = u % BLOCKS, u % 2
            wait(wload(1, j, x))
            dl(u).wait()

            @pl.when(i < LOW - 1)
            def _():
                run(wload(1, (u + 1) % BLOCKS, 1 - x))
                dl(u + 1).start()

            half = u // BLOCKS
            sums = at(half, HALF)
            acc[sums] = jnp.where(j == 0, 0.0, acc[sums]) + _dot(dgu[at(x, HALF)], wgu[x], 1, 1)

            @pl.when(j == BLOCKS - 1)
            def _():
                pl.when(half == 0)(lambda: h1_load().wait())

                def one(t):
                    there = pl.ds(pl.multiple_of(half * HALF + t * 256, 256), 256)
                    wide, da = f(av[there]), acc[there]
                    scale = lax.rsqrt(jnp.mean(wide * wide, -1, keepdims=True) + 1e-6)
                    inner = jnp.mean(wide * da, -1, keepdims=True)
                    back = (scale * da - wide * (scale * scale * scale * inner)).astype(BF)
                    dv[there] = (f(dv[there]) + f(back)).astype(BF)

                loop(0, HALF // 256, one)
                pl.when(half == 1)(lambda: a0_load().start())

        @pl.when(i == LOW - 2)
        def _():
            wdload(0, 0, 0).start()
            run(gl(0))
            run(gl(1))

    x_tile(0).start()
    run(wload(0, 0, 0))
    wdload(0, 0, 0).start()
    run([x_tile(t) for t in range(1, TILES)] + [dy_tile(t) for t in range(TILES)])
    hid[...] = jnp.zeros_like(hid)
    loop(0, STEPS, forward)
    down(STEPS - 1)
    close(TILES - 1)
    for s in range(STEPS - 3, STEPS):
        wait(gl(s, True))
    pl.semaphore_wait(barrier, 2 + jnp.where(more, 1, 0) + jnp.where(less, 1, 0))

    def tick(i):
        before(i)
        compute(i)
        communicate(i - LEAD)

    loop(0, N + LAST + LEAD, tick)


def step_scratch():
    d = pltpu.SemaphoreType.DMA
    ry, rz = ROWS

    def vm(*shape, dtype=BF):
        return pltpu.VMEM(shape, dtype)

    sums = [vm(NS, 2, LINE, r, LANES) for _ in range(2) for r in (ry, rz)]
    lines = [vm(NS, LINE, *r, LANES) for _ in range(2) for r in ((ry,), (2, rz))]
    small = [vm(n, *SHAPE[i], dtype=t) for n, t in ((NL, F32), (NL, F32), (NW, BF)) for i in (UP, DOWN)]
    ring, two, four, three = d((NS,)), d((NS, 2)), d((2, NS, LINE)), d((NS, LINE - 1))
    sems = [two, two, two, ring, ring, four, four, four, four, ring, ring, d((NL, 3)), d((NL, 3))]
    sems += [three] * 4 + [d((NS, 2 * LINE - 1))] * 2 + [three] * 4 + [ring, ring, ring, d((2 * NS,))]
    work = [vm(T, D), vm(T, D), vm(2, D, 2 * FB), vm(2, FB, D), vm(T, FB), vm(T, 2 * FB), vm(2, LINE, 2, D // 16, 2 * FB), vm(16, 40, D)]
    work += [vm(T, D, dtype=F32), vm(3, 2, TT, FB, dtype=F32)]
    work += [d((TILES,)), d((TILES,)), d((2, 2)), d((2,)), d, d((2, 2)), d, d((2,)), d((3, 2)), d, d, d((3, 2)), d((TILES,))]
    return [*sums, *lines, *small, vm(NS, LINE, ry, LANES), vm(NS, rz, LANES), *sems, *work]


def hbm(n):
    return [pl.BlockSpec(memory_space=pl.ANY)] * n


def step_of(x, dy, w, m, v):
    def blocks(t, *tail):
        return (t.shape[0], 2, LINE, 2, *(tail or (t.shape[1] // 16,)), t.shape[-1])

    like = jax.ShapeDtypeStruct
    views = [t.reshape(blocks(t)) for t in w]
    args = [x, dy, *w, *views, *m, *v]
    outs = [like(t.shape, BF) for t in views] + [like(t.shape, F32) for t in (*m, *v)]
    outs += [like(t.shape, BF) for t in views[:DOWN]] + [like(blocks(w[DOWN], 5, 40), BF), like((BLOCKS, T, 2 * FB), BF)]
    outs += [like((T, F), F32)] * 2 + [like((T, D), BF)] * 2
    new = pl.pallas_call(
        step_kernel,
        out_shape=outs,
        in_specs=hbm(len(args)),
        out_specs=hbm(len(outs)),
        scratch_shapes=step_scratch(),
        compiler_params=pltpu.CompilerParams(collective_id=0, has_side_effects=True, vmem_limit_bytes=67043328),
    )(*args)
    old = (*w, *m, *v)
    return copied([n.reshape(t.shape) for n, t in zip(new, old)])


def copy_kernel(n, *refs):
    src, dst, tmp = refs[:n], refs[n : 2 * n], refs[2 * n : 3 * n]
    s_in, s_out = refs[3 * n :]
    cuts = [(k, l, at(b, t.shape[1] // 4)) for k, t in enumerate(src) for l in range(2) for b in range(4 if t.dtype == BF else 0)]
    cuts += [(k, l, ALL) for k, t in enumerate(src) for l in range(2) if t.dtype == F32]
    ins = [near(src[k].at[l, r], tmp[k].at[l, r], s_in.at[e]) for e, (k, l, r) in enumerate(cuts)]
    outs = [near(tmp[k].at[l, r], dst[k].at[l, r], s_out.at[e]) for e, (k, l, r) in enumerate(cuts)]
    run(ins)
    for i, o in zip(ins, outs, strict=True):
        i.wait()
        o.start()
    wait(outs)


def copied(arrays):
    n = len(arrays)
    many = sum(8 if t.dtype == BF else 2 for t in arrays)
    return pl.pallas_call(
        functools.partial(copy_kernel, n),
        out_shape=[jax.ShapeDtypeStruct(t.shape, t.dtype) for t in arrays],
        in_specs=hbm(n),
        out_specs=hbm(n),
        scratch_shapes=[pltpu.VMEM(t.shape, t.dtype) for t in arrays] + [pltpu.SemaphoreType.DMA((many,))] * 2,
        compiler_params=pltpu.CompilerParams(vmem_limit_bytes=67043328),
    )(*arrays)


def solution(mesh):
    def step(x, dy, *arrays):
        w, m, v = (arrays[i : i + 3] for i in (0, 3, 6))
        return tuple(step_of(x[0], dy[0], w, m, v))

    one, whole, rows = P(("rep", "dp")), P(), P(None, "dp")
    return jax.shard_map(
        step,
        mesh=mesh,
        in_specs=(one, one) + (whole,) * 3 + (rows,) * 6,
        out_specs=(P("rep"),) * 3 + (P("rep", "dp"),) * 6,
        check_vma=False,
    )
```

```python
import functools

import jax
import jax.numpy as jnp
from jax import lax
from jax.experimental import pallas as pl
from jax.experimental.pallas import tpu as pltpu
from jax.sharding import PartitionSpec as P

BF, F32 = jnp.bfloat16, jnp.float32
MESH = pl.DeviceIdType.MESH
ALL = slice(None)
T, D, F, FB, LANES = 2048, 1024, 3200, 640, 128
BLOCKS = F // FB
TT, TILES = 512, 4
HALF = T // 2
LINE = 4
NS = 8
NL, NW = 4, 16
LAST = 11
LEAD = 3
GATE, UP, DOWN = range(3)
SHAPE = {GATE: (32, FB), UP: (32, FB), DOWN: (40, 512)}
FIRST = {GATE: (32, 384), UP: (32, 384), DOWN: (24, 512)}
MANY = 2
ROWS = (96, 64)
NGU, ND = 20, 10
N = 2 * (NGU + ND)
DA, LOW = 4 * BLOCKS, 4 * BLOCKS + 2 * BLOCKS
END = LOW + 4 * BLOCKS


def _dot(p, q, cp, cq):
    return lax.dot_general(p, q, (((cp,), (cq,)), ((), ())), preferred_element_type=F32)


def f(x):
    return x.astype(F32)


def near(src, dst, sem):
    return pltpu.make_async_copy(src, dst, sem)


def at(k, size):
    return pl.ds(pl.multiple_of(k * size, size), size)


def loop(lo, hi, do):
    def one(d, _):
        do(d)
        return 0

    lax.fori_loop(lo, hi, one, 0)


def run(copies):
    for c in copies:
        c.start()


def wait(copies):
    for c in copies:
        c.wait()


def pieces(kind):
    (r, c), (r0, c0) = SHAPE[kind], FIRST[kind]
    if kind < DOWN:
        left = c0 // LANES
        return [(0, i * r, r, 0, i) for i in range(left)] + [(1, (i - left) * r, r, 0, i) for i in range(left, c // LANES)]
    return [(p, i * k, k, o, i) for p, k, o in ((0, r0, 0), (1, r - r0, r0)) for i in range(c // LANES)]


def cut(kind, s, part=None):
    (r, c), (r0, c0) = SHAPE[kind], FIRST[kind]
    row, col = (s % MANY, s // MANY) if kind < DOWN else (s // MANY, s % MANY)
    row, col = pl.multiple_of(row * r, 8), pl.multiple_of(col * c, LANES)
    if part is None:
        return pl.ds(row, r), pl.ds(col, c)
    if kind < DOWN:
        return pl.ds(row, r), pl.ds(col + c0, c - c0) if part else pl.ds(col, c0)
    return pl.ds(row + r0, r - r0) if part else pl.ds(row, r0), pl.ds(col, c)


def step_kernel(*refs):
    refs = list(refs)

    def take(n):
        out = refs[:n]
        del refs[:n]
        return out

    x, dy = take(2)
    nat, w, m, v, ow, om, ov = (take(3) for _ in range(7))
    g_gu, g_down = take(2)
    dgu_all, gate0, up0, a0, h1 = take(5)
    own, oth, rr, ll, mbuf, vbuf, wbuf = (take(2) for _ in range(7))
    (ry, ryz, s_own, s_e, r_e, s_y, r_y, s_zr, r_zr, s_zl, r_zl, s_yz, r_yz, s_ld, s_st, s_ag, r_ag, s_c, r_c,
     av, dv, wgu, wd, hid, dgu, gout, dout, acc, gt,
     s_x, s_dy, s_w, s_wd, s_dgu, s_go, s_do, s_dl, s_gt, s_h, s_a0, s_keep, s_h1) = refs
    rep, dp = lax.axis_index("rep"), lax.axis_index("dp")
    c, z, y = dp % 2, (dp // 2) % LINE, dp // (2 * LINE)
    core, across, right, left = dp + 1 - 2 * c, dp + (1 - 2 * y) * 2 * LINE, dp + 2, dp - 2
    more, less = z < LINE - 1, z > 0

    def far(src, dst, ss, rs, to):
        return pltpu.make_async_remote_copy(src_ref=src, dst_ref=dst, send_sem=ss, recv_sem=rs, device_id=(rep, to), device_id_type=MESH)

    def clear(bufs):
        for b in bufs:
            b[...] = jnp.zeros_like(b)

    pl.when(z == 0)(lambda: clear(rr))
    pl.when(z == LINE - 1)(lambda: clear(ll))
    barrier = pltpu.get_barrier_semaphore()

    def greet(to):
        pl.semaphore_signal(barrier, inc=1, device_id=(rep, to), device_id_type=MESH)

    greet(core)
    greet(across)
    pl.when(more)(lambda: greet(right))
    pl.when(less)(lambda: greet(left))
    def what(k):
        u = k % (NGU + ND)
        gu = u < NGU
        return 1 - k // (NGU + ND), jnp.where(gu, (u // 2) % 2, DOWN), jnp.where(gu, (u // 4) * 2 + u % 2, u - NGU)

    def each(kind, do):
        def one(i):
            do(i)

        for i in SHAPE:
            pl.when(kind == i)(functools.partial(one, i))

    def chip(do):
        def one(zz):
            do(zz)

        for zz in range(LINE):
            pl.when(z == zz)(functools.partial(one, zz))

    def stage(tick, st, do):
        k = tick - st
        pl.when((k >= 0) & (k < N))(lambda: do(k, k % NS))

    def fetch(k, q):
        layer, kind, s = what(k)

        def both(src, dst, part):
            near(src(c), own[part].at[dst], s_own.at[q, part]).start()
            far(src(1 - c), oth[part].at[dst], s_e.at[q, part], r_e.at[q, part], core).start()

        @pl.when(kind < DOWN)
        def _():
            for part, d0 in enumerate((0, ROWS[0])):
                both(lambda h: g_gu.at[layer, s // MANY, :, kind, s % MANY, :, h, pl.ds(d0, ROWS[part])], q, part)

        @pl.when(kind == DOWN)
        def _():
            cols = cut(DOWN, s)[1].start
            for part, d0, n, s0, col in pieces(DOWN):
                here = (s // MANY, pl.ds(s0, n), pl.ds(cols + col * LANES, LANES))
                both(lambda h: g_down.at[(layer, ALL, ALL, h, *here)], (q, ALL, ALL, pl.ds(d0, n)), part)

    def exchange(q, part):
        return far(own[part].at[q], oth[part].at[q], s_e.at[q, part], r_e.at[q, part], core)

    def y_send(q):
        return far(own[0].at[q, 1 - y], ry.at[q], s_y.at[q], r_y.at[q], across)

    def first(k, q):
        for part in range(2):
            near(own[part].at[q], own[part].at[q], s_own.at[q, part]).wait()
            exchange(q, part).wait_recv()

        def add(d):
            own[0][q, 1 - y, d] = (f(own[0][q, 1 - y, d]) + f(oth[0][q, 1 - y, d])).astype(BF)

        loop(0, LINE, add)
        y_send(q).start()

    def span(zz, to_right):
        return (zz + 1, LINE) if to_right else (0, zz)

    def line(part, q, zz, to_right):
        ss, rs, buf, to = (s_zr, r_zr, rr, right) if to_right else (s_zl, r_zl, ll, left)
        lo, hi = span(zz, to_right)
        d = pl.ds(lo, hi - lo)
        src, dst = (own[0].at[q, y, d], buf[0].at[q, d]) if part == 0 else (own[1].at[q, :, d], buf[1].at[q, :, d])
        return far(src, dst, ss.at[part, q], rs.at[part, q], to)

    def total(part, q, d, buf):
        if part == 0:
            own[0][q, y, d] = (f(own[0][q, y, d]) + f(oth[0][q, y, d]) + f(ry[q, d]) + f(buf[0][q, d])).astype(BF)
        else:
            for j in range(2):
                own[1][q, j, d] = (f(own[1][q, j, d]) + f(oth[1][q, j, d]) + f(buf[1][q, j, d])).astype(BF)

    def go(to_right, part, zz, k, q):
        back = zz - 1 if to_right else zz + 1
        if 0 <= back < LINE:
            line(part, q, back, to_right).wait_recv()
        lo, hi = span(zz, to_right)
        for d in range(lo, hi):
            total(part, q, d, rr if to_right else ll)
        if lo < hi:
            line(part, q, zz, to_right).start()

    def lines(i, zz):
        for part in (1, 0):
            for to_right, steps in ((True, zz), (False, LINE - 1 - zz)):
                stage(i, 1 - part + steps, functools.partial(go, to_right, part, zz))

    def yz_send(q):
        return far(own[1].at[q, 1 - y, z], ryz.at[q], s_yz.at[q], r_yz.at[q], across)

    def yz(k, q):
        b = (q, 1 - y, z)
        own[1][b] = (f(own[1][b]) + f(oth[1][b]) + f(rr[1][b]) + f(ll[1][b])).astype(BF)
        yz_send(q).start()

    def small(i, k, put):
        layer, _, s = what(k)
        rows, cols = cut(i, s)
        e, t = k % NL, i // DOWN
        block = (layer, y, z, c, rows, cols)
        there = ((om if put else m)[i].at[layer, rows, cols], (ov if put else v)[i].at[layer, rows, cols], (ow if put else w)[i].at[block])
        here = (mbuf[t].at[e], vbuf[t].at[e], wbuf[t].at[k % NW])
        sems = s_st if put else s_ld
        return [near(b, r, sems.at[e, h]) if put else near(r, b, sems.at[e, h]) for h, (r, b) in enumerate(zip(there, here, strict=True))]

    def final(k, q):
        yz_send(q).wait_recv()

        def of(i):
            wait(small(i, k, False))
            mb, vb, wb = (b[i // DOWN] for b in (mbuf, vbuf, wbuf))
            for part, d0, n, s0, col in pieces(i):
                r = pl.ds(d0, n)
                gr = f(own[part][q, y, z, r]) + f(oth[part][q, y, z, r])
                gr += f(ry[q, z, r]) + f(rr[0][q, z, r]) + f(ll[0][q, z, r]) if part == 0 else f(rr[1][q, y, z, r]) + f(ll[1][q, y, z, r]) + f(ryz[q, r])
                gr = f(gr.astype(BF))
                b = (pl.ds(s0, n), pl.ds(col * LANES, LANES))
                bm, bw = (k % NL, *b), (k % NW, *b)
                mm = 0.9 * mb[bm] + 0.1 * gr
                vv = 0.95 * vb[bm] + 0.05 * gr * gr
                ww = f(wb[bw])
                mb[bm] = mm
                vb[bm] = vv
                wb[bw] = (ww - 0.02 * (mm * lax.rsqrt(vv + 1e-8) + 0.1 * ww)).astype(BF)
            run(small(i, k, True))

        each(what(k)[1], of)

    def move(e, i, k, q, zz):
        layer, _, s = what(k)
        part = e // 3
        along = e % 4
        lo, hi = (0, zz + 1) if e in (0, 4) else (zz, LINE) if e in (1, 5) else (0, LINE) if part == 0 else (zz, zz + 1)
        blocks = lo if hi - lo == 1 else pl.ds(lo, hi - lo)
        dst = ow[i].at[(layer, ALL if e > 3 else y, blocks, c, *cut(i, s, part))]
        src = dst
        if hi - lo == 1 and e < 4:
            (r, cc), (r0, c0) = SHAPE[i], FIRST[i]
            rows = (pl.ds(r0, r - r0) if part else pl.ds(0, r0)) if i == DOWN else pl.ds(0, r)
            cols = pl.ds(0, cc) if i == DOWN else pl.ds(c0, cc - c0) if part else pl.ds(0, c0)
            src = wbuf[i // DOWN].at[k % NW, rows, cols]
        to = (right, left)[along] if along < 2 else across
        return far(src, dst, s_ag.at[e, q], r_ag.at[e, q], to)

    def events(zz):
        side = LINE - 1
        turn = max(zz, side - zz)
        out = [(0, None, 3), (1, (3, zz), None), (turn, None, 2), (turn + 1, (2, zz), None)]
        for part in range(2):
            for t, back, e, more_ in ((zz, zz - 1, 0, zz < side), (side - zz, zz + 1, 1, zz > 0)):
                e += 4 * part
                out.insert(0, (t + part, (e, back) if 0 <= back < LINE else None, e if more_ else None))
        return out

    def spread(t, zz, k, q):
        todo = [(w_, e) for step, w_, e in events(zz) if step == t]
        if t == 1:
            wait(small(GATE, k, True))
        for w_, _ in todo:
            if w_:
                move(w_[0], GATE, k, q, w_[1]).wait_recv()
        sends = [e for _, e in todo if e is not None]
        if sends:
            each(what(k)[1], lambda i: run([move(e, i, k, q, zz) for e in sends]))

    def over(i, k, q):
        layer, _, s = what(k)
        b = ow[i].at[(layer, ALL, ALL, c, *cut(i, s))]
        return far(b, b, s_c.at[q], r_c.at[k % (2 * NS)], core)

    def hand(k, q):
        each(what(k)[1], lambda i: over(i, k, q).start())

    def finish(zz, k, q):
        over(GATE, k, q).wait()
        for _, _, e in events(zz):
            if e is not None:
                move(e, GATE, k, q, zz).wait_send()

    def sent(zz, k, q):
        for part in range(2):
            exchange(q, part).wait_send()
            for to_right in (True, False):
                lo, hi = span(zz, to_right)
                if lo < hi:
                    line(part, q, zz, to_right).wait_send()
        y_send(q).wait_send()
        yz_send(q).wait_send()

    def spreads(i, zz):
        for t in range(LINE + 1):
            stage(i, LINE + t, functools.partial(spread, t, zz))
        stage(i, NS - 2, functools.partial(sent, zz))
        stage(i, LAST - 1, functools.partial(finish, zz))

    def communicate(i):
        stage(i, 0, first)
        stage(i, 1, lambda k, q: y_send(q).wait_recv())
        chip(lambda zz: lines(i, zz))
        stage(i, LINE - 1, yz)
        stage(i, LINE - 2, lambda k, q: each(what(k)[1], lambda e: run(small(e, k, False))))
        stage(i, LINE, final)
        chip(lambda zz: spreads(i, zz))
        stage(i, 2 * LINE, hand)

    def wload(layer, j, x):
        return [near(nat[h].at[layer, :, at(j, FB)], wgu.at[x, :, pl.ds(FB * h, FB)], s_w.at[x, h]) for h in range(2)]

    def wdload(layer, j, x):
        return near(nat[DOWN].at[layer, at(j, FB)], wd.at[x], s_wd.at[x])

    def x_tile(t):
        return near(x.at[at(t, TT)], dgu.at[at(t, TT), pl.ds(0, D)], s_x.at[t])

    def h1_tile(t):
        return near(dgu.at[at(t, TT), pl.ds(0, D)], h1.at[at(t, TT)], s_h1.at[t])

    def dy_tile(t):
        return near(dy.at[at(t, TT)], dv.at[at(t, TT)], s_dy.at[t])

    def a0_load():
        return near(a0, av, s_a0)

    def a0_keep():
        return near(av, a0, s_a0)

    def keep(j):
        return near(dgu, dgu_all.at[j], s_dgu)

    def dl(u):
        return near(dgu_all.at[u % BLOCKS, at(u // BLOCKS, HALF)], dgu.at[at(u % 2, HALF)], s_dl.at[u % 2])

    def gl(s, put=False):
        e = s % 3
        here = [(t.at[at(s % TILES, TT), at(s // TILES, FB)], gt.at[e, h]) for h, t in enumerate((gate0, up0))]
        return [near(b, t, s_keep.at[e, h]) if put else near(t, b, s_gt.at[e, h]) for h, (t, b) in enumerate(here)]

    def h1_load():
        return near(h1, av, s_h)

    def g_out(layer, j, t):
        return near(gout.at[t], g_gu.at[layer, j, t], s_go.at[t])

    def _rms(b):
        wide = f(b)
        return (wide * lax.rsqrt(jnp.mean(wide * wide, -1, keepdims=True) + 1e-6)).astype(BF)

    def down(s):
        rows, j = at(s % TILES, TT), s // TILES
        acc[rows] = jnp.where(j == 0, 0.0, acc[rows]) + _dot(hid[at(s % 2, TT)], wd[j % 2], 1, 0)

    def close(t):
        rows = at(t, TT)
        new = (f(dgu[rows, :D]) + f(acc[rows].astype(BF))).astype(BF)
        dgu[rows, :D] = new
        av[rows] = _rms(new)
        h1_tile(t).start()

    STEPS = BLOCKS * TILES

    def forward(closing, s):
        j, t = s // TILES, s % TILES
        k = j % 2
        rows = at(t, TT)

        @pl.when(t == 0)
        def _():
            wait(wload(0, j, k))
            wdload(0, j, k).wait()

        @pl.when(t == 1)
        def _():
            last = j == BLOCKS - 1
            layer, nxt = jnp.where(last, 1, 0), jnp.where(last, 0, j + 1)
            run(wload(layer, nxt, 1 - k))
            wdload(layer, nxt, 1 - k).start()

        pl.when(s == TILES)(lambda: a0_keep().start())
        pl.when(s == STEPS - TILES)(lambda: a0_keep().wait())
        pl.when(s >= 3)(lambda: wait(gl(s - 3, True)))
        gu = _dot(av[rows], wgu[k], 1, 0)
        down(jnp.where(s == 0, TILES - 1, s - 1))
        gate, up = gu[:, :FB], gu[:, FB:]
        gt[s % 3, 0] = gate
        gt[s % 3, 1] = up
        hid[at(s % 2, TT)] = (gate * jax.nn.sigmoid(gate) * up).astype(BF)
        if closing:
            close(t - 1)
        run(gl(s, True))

    def gated(rows, gate, up, dh):
        s = jax.nn.sigmoid(gate)
        gs = gate * s
        dh = f(dh.astype(BF))
        hid[rows] = (gs * up).astype(BF)
        dgu[rows, FB:] = (dh * gs).astype(BF)
        dgu[rows, :FB] = (dh * up * (s + gs * (1 - s))).astype(BF)

    def gu_half(t, layer, j):
        out = _dot(av[:, at(t, TT)], dgu[...], 0, 0).astype(BF)
        many = FB // LANES
        r = SHAPE[GATE][0]
        for n in range(2 * many):
            part = out[:, LANES * n : LANES * (n + 1)].reshape(LINE, 2, MANY, r, LANES)
            for b in range(MANY):
                gout[t, n // many, b, :, :, pl.ds(n % many * r, r)] = part[:, :, b]
        g_out(layer, j, t).start()

    def where(i):
        top, low = i < DA, (i >= LOW) & (i < END)
        ii = jnp.where(top, i, i - LOW)
        return top, low, ii // 4, ii % 4, jnp.where(top, 1, 0)

    def before(i):
        top, low, j, r, layer = where(i)

        @pl.when((top | low) & (r == 3))
        def _():
            wait([g_out(layer, j, t) for t in range(2)])

        stage(i, LEAD, fetch)

    def compute(i):
        top, low, j, r, layer = where(i)
        x = jnp.where(top, j + 1, j) % 2

        pl.when(((i > 4) & (i <= DA + 1) & (i % 4 == 1)) | ((i > LOW + 4) & (i <= END + 1) & (i % 4 == (LOW + 1) % 4)))(lambda: near(dout, dout, s_do).wait())

        @pl.when(top & (r == 0))
        def _():
            wait(wload(1, j, x))
            wdload(1, j, x).wait()
            pl.when(j > 0)(lambda: keep(j - 1).wait())

            @pl.when(j < BLOCKS - 1)
            def _():
                run(wload(1, j + 1, 1 - x))
                wdload(1, j + 1, 1 - x).start()

        @pl.when(top & (r < 2))
        def _():
            @pl.when(j == 0)
            def _():
                for t in range(2):
                    wait((dy_tile(2 * r + t), h1_tile(2 * r + t)))

            def one(t):
                rows = at(t, TT)
                gu = _dot(av[rows], wgu[x], 1, 0)
                gated(rows, gu[:, :FB], gu[:, FB:], _dot(dv[rows], wd[x], 1, 1))

            loop(2 * r, 2 * r + 2, one)
            pl.when(r == 1)(lambda: keep(j).start())

        @pl.when(low & (r == 0))
        def _():
            wdload(0, j, x).wait()
            pl.when(j < BLOCKS - 1)(lambda: wdload(0, j + 1, 1 - x).start())

        @pl.when(low & (r < 2))
        def _():
            def one(t):
                s = TILES * j + t
                wait(gl(s))
                pl.when(s < BLOCKS * TILES - 2)(lambda: run(gl(s + 2)))
                rows = at(t, TT)
                gated(rows, gt[s % 3, 0], gt[s % 3, 1], _dot(dv[rows], wd[x], 1, 1))

            loop(3 * r, 3 + r, one)

        @pl.when((top & (r == 2)) | (low & ((r == 1) | (r == 2))))
        def _():
            pl.when(i == LOW + 1)(lambda: a0_load().wait())
            loop(jnp.where(top, 0, r - 1), jnp.where(top, 2, r), lambda t: gu_half(t, layer, j))

        @pl.when((top | low) & (r == 3))
        def _():
            out = _dot(hid[...], dv[...], 0, 0)
            pp, n = dout.shape[:2]
            for p in range(pp):
                dout[p] = out[n * p : n * (p + 1)].astype(BF)

            def send(p):
                o = pp * j + p
                near(dout.at[p], g_down.at[layer, o // 40, (o // 10) % LINE, (o // 5) % 2, o % 5], s_do).start()

            loop(0, pp, send)

        @pl.when(i == DA - 1)
        def _():
            keep(BLOCKS - 1).wait()
            run(wload(1, 0, 0))
            dl(0).start()
            h1_load().start()

        @pl.when((i >= DA) & (i < LOW))
        def _():
            u = i - DA
            j, x = u % BLOCKS, u % 2
            wait(wload(1, j, x))
            dl(u).wait()

            @pl.when(i < LOW - 1)
            def _():
                run(wload(1, (u + 1) % BLOCKS, 1 - x))
                dl(u + 1).start()

            half = u // BLOCKS
            sums = at(half, HALF)
            acc[sums] = jnp.where(j == 0, 0.0, acc[sums]) + _dot(dgu[at(x, HALF)], wgu[x], 1, 1)

            @pl.when(j == BLOCKS - 1)
            def _():
                pl.when(half == 0)(lambda: h1_load().wait())

                def one(t):
                    there = pl.ds(pl.multiple_of(half * HALF + t * 256, 256), 256)
                    wide, da = f(av[there]), acc[there]
                    scale = lax.rsqrt(jnp.mean(wide * wide, -1, keepdims=True) + 1e-6)
                    inner = jnp.mean(wide * da, -1, keepdims=True)
                    back = (scale * da - wide * (scale * scale * scale * inner)).astype(BF)
                    dv[there] = (f(dv[there]) + f(back)).astype(BF)

                loop(0, HALF // 256, one)
                pl.when(half == 1)(lambda: a0_load().start())

        @pl.when(i == LOW - 2)
        def _():
            wdload(0, 0, 0).start()
            run(gl(0))
            run(gl(1))

    x_tile(0).start()
    run(wload(0, 0, 0))
    wdload(0, 0, 0).start()
    run([x_tile(t) for t in range(1, TILES)] + [dy_tile(t) for t in range(TILES)])
    hid[...] = jnp.zeros_like(hid)

    def norm(t):
        x_tile(t).wait()
        av[at(t, TT)] = _rms(dgu[at(t, TT), :D])

    loop(0, TILES, norm)
    loop(0, STEPS - TILES + 1, functools.partial(forward, False))
    loop(STEPS - TILES + 1, STEPS, functools.partial(forward, True))
    down(STEPS - 1)
    close(TILES - 1)
    for s in range(STEPS - 3, STEPS):
        wait(gl(s, True))
    pl.semaphore_wait(barrier, 2 + jnp.where(more, 1, 0) + jnp.where(less, 1, 0))

    def tick(i):
        before(i)
        compute(i)
        communicate(i - LEAD)

    loop(0, N + LAST + LEAD, tick)


def step_scratch():
    d = pltpu.SemaphoreType.DMA
    ry, rz = ROWS

    def vm(*shape, dtype=BF):
        return pltpu.VMEM(shape, dtype)

    sums = [vm(NS, 2, LINE, r, LANES) for _ in range(2) for r in (ry, rz)]
    lines = [vm(NS, *r, LANES) for _ in range(2) for r in ((LINE, ry), (2, LINE, rz))]
    small = [vm(n, *SHAPE[i], dtype=t) for n, t in ((NL, F32), (NL, F32), (NW, BF)) for i in (UP, DOWN)]
    ring, two, parts, six = d((NS,)), d((NS, 2)), d((2, NS)), d((6, NS))
    sems = [two, two, two, ring, ring, parts, parts, parts, parts, ring, ring, d((NL, 3)), d((NL, 3)), six, six, ring, d((2 * NS,))]
    work = [vm(T, D), vm(T, D), vm(2, D, 2 * FB), vm(2, FB, D), vm(T, FB), vm(T, 2 * FB), vm(2, 2, MANY, LINE, 2, ry + rz, LANES), vm(16, 40, D)]
    work += [vm(T, D, dtype=F32), vm(3, 2, TT, FB, dtype=F32)]
    work += [d((TILES,)), d((TILES,)), d((2, 2)), d((2,)), d, d((2,)), d, d((2,)), d((3, 2)), d, d, d((3, 2)), d((TILES,))]
    return [*sums, *lines, *small, vm(NS, LINE, ry, LANES), vm(NS, rz, LANES), *sems, *work]


def hbm(n):
    return [pl.BlockSpec(memory_space=pl.ANY)] * n


def step_of(x, dy, w, m, v):
    def blocks(t, *tail):
        return (t.shape[0], 2, LINE, 2, *(tail or (t.shape[1] // 16,)), t.shape[-1])

    like = jax.ShapeDtypeStruct
    views = [t.reshape(blocks(t)) for t in w]
    args = [x, dy, *w, *views, *m, *v]
    outs = [like(t.shape, BF) for t in views] + [like(t.shape, F32) for t in (*m, *v)]
    outs += [like((2, BLOCKS, 2, 2, MANY, LINE, 2, sum(ROWS), LANES), BF), like(blocks(w[DOWN], 5, 40), BF), like((BLOCKS, T, 2 * FB), BF)]
    outs += [like((T, F), F32)] * 2 + [like((T, D), BF)] * 2
    new = pl.pallas_call(
        step_kernel,
        out_shape=outs,
        in_specs=hbm(len(args)),
        out_specs=hbm(len(outs)),
        scratch_shapes=step_scratch(),
        compiler_params=pltpu.CompilerParams(collective_id=0, has_side_effects=True, vmem_limit_bytes=67043328),
    )(*args)
    old = (*w, *m, *v)
    return copied([n.reshape(t.shape) for n, t in zip(new, old)])


def copy_kernel(n, *refs):
    src, dst, tmp = refs[:n], refs[n : 2 * n], refs[2 * n : 3 * n]
    s_in, s_out = refs[3 * n :]
    cuts = [(k, l, at(b, t.shape[1] // 4)) for k, t in enumerate(src) for l in range(2) for b in range(4 if t.dtype == BF else 0)]
    cuts += [(k, l, ALL) for k, t in enumerate(src) for l in range(2) if t.dtype == F32]
    ins = [near(src[k].at[l, r], tmp[k].at[l, r], s_in.at[e]) for e, (k, l, r) in enumerate(cuts)]
    outs = [near(tmp[k].at[l, r], dst[k].at[l, r], s_out.at[e]) for e, (k, l, r) in enumerate(cuts)]
    run(ins)
    for i, o in zip(ins, outs, strict=True):
        i.wait()
        o.start()
    wait(outs)


def copied(arrays):
    n = len(arrays)
    many = sum(8 if t.dtype == BF else 2 for t in arrays)
    return pl.pallas_call(
        functools.partial(copy_kernel, n),
        out_shape=[jax.ShapeDtypeStruct(t.shape, t.dtype) for t in arrays],
        in_specs=hbm(n),
        out_specs=hbm(n),
        scratch_shapes=[pltpu.VMEM(t.shape, t.dtype) for t in arrays] + [pltpu.SemaphoreType.DMA((many,))] * 2,
        compiler_params=pltpu.CompilerParams(vmem_limit_bytes=67043328),
    )(*arrays)


def solution(mesh):
    def step(x, dy, *arrays):
        w, m, v = (arrays[i : i + 3] for i in (0, 3, 6))
        return tuple(step_of(x[0], dy[0], w, m, v))

    one, whole, rows = P(("rep", "dp")), P(), P(None, "dp")
    return jax.shard_map(
        step,
        mesh=mesh,
        in_specs=(one, one) + (whole,) * 3 + (rows,) * 6,
        out_specs=(P("rep"),) * 3 + (P("rep", "dp"),) * 6,
        check_vma=False,
    )
```

```python
import functools

import jax
import jax.numpy as jnp
from jax import lax
from jax.experimental import pallas as pl
from jax.experimental.pallas import tpu as pltpu
from jax.sharding import PartitionSpec as P

BF, F32 = jnp.bfloat16, jnp.float32
MESH = pl.DeviceIdType.MESH
ALL = slice(None)
T, D, F, FB, LANES = 2048, 1024, 3200, 640, 128
BLOCKS = F // FB
TT, TILES = 512, 4
HALF = T // 2
LINE = 4
NS = 8
NL, NW = 4, 16
LAST = 11
LEAD = 3
GATE, UP, DOWN = range(3)
SHAPE = {GATE: (32, FB), UP: (32, FB), DOWN: (40, 512)}
FIRST = {GATE: (32, 384), UP: (32, 384), DOWN: (24, 512)}
MANY = 2
ROWS = (96, 64)
NGU, ND = 20, 10
N = 2 * (NGU + ND)
DA, LOW = 4 * BLOCKS, 4 * BLOCKS + 2 * BLOCKS
END = LOW + 4 * BLOCKS


def _dot(p, q, cp, cq):
    return lax.dot_general(p, q, (((cp,), (cq,)), ((), ())), preferred_element_type=F32)


def f(x):
    return x.astype(F32)


def near(src, dst, sem):
    return pltpu.make_async_copy(src, dst, sem)


def at(k, size):
    return pl.ds(pl.multiple_of(k * size, size), size)


def loop(lo, hi, do):
    def one(d, _):
        do(d)
        return 0

    lax.fori_loop(lo, hi, one, 0)


def run(copies):
    for c in copies:
        c.start()


def wait(copies):
    for c in copies:
        c.wait()


def pieces(kind):
    (r, c), (r0, c0) = SHAPE[kind], FIRST[kind]
    if kind < DOWN:
        left = c0 // LANES
        return [(0, i * r, r, 0, i) for i in range(left)] + [(1, (i - left) * r, r, 0, i) for i in range(left, c // LANES)]
    return [(p, i * k, k, o, i) for p, k, o in ((0, r0, 0), (1, r - r0, r0)) for i in range(c // LANES)]


def cut(kind, s, part=None):
    (r, c), (r0, c0) = SHAPE[kind], FIRST[kind]
    row, col = (s % MANY, s // MANY) if kind < DOWN else (s // MANY, s % MANY)
    row, col = pl.multiple_of(row * r, 8), pl.multiple_of(col * c, LANES)
    if part is None:
        return pl.ds(row, r), pl.ds(col, c)
    if kind < DOWN:
        return pl.ds(row, r), pl.ds(col + c0, c - c0) if part else pl.ds(col, c0)
    return pl.ds(row + r0, r - r0) if part else pl.ds(row, r0), pl.ds(col, c)


def step_kernel(*refs):
    refs = list(refs)

    def take(n):
        out = refs[:n]
        del refs[:n]
        return out

    x, dy = take(2)
    nat, w, m, v, ow, om, ov = (take(3) for _ in range(7))
    g_gu, g_down = take(2)
    dgu_all, gate0, up0, a0, h1 = take(5)
    own, oth, rr, ll, mbuf, vbuf, wbuf = (take(2) for _ in range(7))
    (ry, ryz, s_own, s_e, r_e, s_y, r_y, s_zr, r_zr, s_zl, r_zl, s_yz, r_yz, s_ld, s_st, s_ag, r_ag, s_c, r_c,
     av, dv, wgu, wd, hid, dgu, gout, dout, acc, gt,
     s_x, s_dy, s_w, s_wd, s_dgu, s_go, s_do, s_dl, s_gt, s_h, s_a0, s_keep, s_h1) = refs
    rep, dp = lax.axis_index("rep"), lax.axis_index("dp")
    c, z, y = dp % 2, (dp // 2) % LINE, dp // (2 * LINE)
    core, across, right, left = dp + 1 - 2 * c, dp + (1 - 2 * y) * 2 * LINE, dp + 2, dp - 2
    more, less = z < LINE - 1, z > 0

    def far(src, dst, ss, rs, to):
        return pltpu.make_async_remote_copy(src_ref=src, dst_ref=dst, send_sem=ss, recv_sem=rs, device_id=(rep, to), device_id_type=MESH)

    def clear(bufs):
        for b in bufs:
            b[...] = jnp.zeros_like(b)

    pl.when(z == 0)(lambda: clear(rr))
    pl.when(z == LINE - 1)(lambda: clear(ll))
    barrier = pltpu.get_barrier_semaphore()

    def greet(to):
        pl.semaphore_signal(barrier, inc=1, device_id=(rep, to), device_id_type=MESH)

    greet(core)
    greet(across)
    pl.when(more)(lambda: greet(right))
    pl.when(less)(lambda: greet(left))
    def what(k):
        u = k % (NGU + ND)
        gu = u < NGU
        return 1 - k // (NGU + ND), jnp.where(gu, (u // 2) % 2, DOWN), jnp.where(gu, (u // 4) * 2 + u % 2, u - NGU)

    def each(kind, do):
        def one(i):
            do(i)

        for i in SHAPE:
            pl.when(kind == i)(functools.partial(one, i))

    def chip(do):
        def one(zz):
            do(zz)

        for zz in range(LINE):
            pl.when(z == zz)(functools.partial(one, zz))

    def stage(tick, st, do):
        k = tick - st
        pl.when((k >= 0) & (k < N))(lambda: do(k, k % NS))

    def fetch(k, q):
        layer, kind, s = what(k)

        def both(src, dst, part):
            near(src(c), own[part].at[dst], s_own.at[q, part]).start()
            far(src(1 - c), oth[part].at[dst], s_e.at[q, part], r_e.at[q, part], core).start()

        @pl.when(kind < DOWN)
        def _():
            for part, d0 in enumerate((0, ROWS[0])):
                both(lambda h: g_gu.at[layer, s // MANY, :, kind, s % MANY, :, h, pl.ds(d0, ROWS[part])], q, part)

        @pl.when(kind == DOWN)
        def _():
            cols = cut(DOWN, s)[1].start
            for part, d0, n, s0, col in pieces(DOWN):
                here = (s // MANY, pl.ds(s0, n), pl.ds(cols + col * LANES, LANES))
                both(lambda h: g_down.at[(layer, ALL, ALL, h, *here)], (q, ALL, ALL, pl.ds(d0, n)), part)

    def exchange(q, part):
        return far(own[part].at[q], oth[part].at[q], s_e.at[q, part], r_e.at[q, part], core)

    def y_send(q):
        return far(own[0].at[q, 1 - y], ry.at[q], s_y.at[q], r_y.at[q], across)

    def first(k, q):
        for part in range(2):
            near(own[part].at[q], own[part].at[q], s_own.at[q, part]).wait()
            exchange(q, part).wait_recv()

        def add(d):
            own[0][q, 1 - y, d] = (f(own[0][q, 1 - y, d]) + f(oth[0][q, 1 - y, d])).astype(BF)

        loop(0, LINE, add)
        y_send(q).start()

    def span(zz, to_right):
        return (zz + 1, LINE) if to_right else (0, zz)

    def line(part, q, zz, to_right):
        ss, rs, buf, to = (s_zr, r_zr, rr, right) if to_right else (s_zl, r_zl, ll, left)
        lo, hi = span(zz, to_right)
        d = pl.ds(lo, hi - lo)
        src, dst = (own[0].at[q, y, d], buf[0].at[q, d]) if part == 0 else (own[1].at[q, :, d], buf[1].at[q, :, d])
        return far(src, dst, ss.at[part, q], rs.at[part, q], to)

    def total(part, q, d, buf):
        if part == 0:
            own[0][q, y, d] = (f(own[0][q, y, d]) + f(oth[0][q, y, d]) + f(ry[q, d]) + f(buf[0][q, d])).astype(BF)
        else:
            for j in range(2):
                own[1][q, j, d] = (f(own[1][q, j, d]) + f(oth[1][q, j, d]) + f(buf[1][q, j, d])).astype(BF)

    def go(to_right, part, zz, k, q):
        back = zz - 1 if to_right else zz + 1
        if 0 <= back < LINE:
            line(part, q, back, to_right).wait_recv()
        lo, hi = span(zz, to_right)
        for d in range(lo, hi):
            total(part, q, d, rr if to_right else ll)
        if lo < hi:
            line(part, q, zz, to_right).start()

    def lines(i, zz):
        for part in (1, 0):
            for to_right, steps in ((True, zz), (False, LINE - 1 - zz)):
                stage(i, 1 - part + steps, functools.partial(go, to_right, part, zz))

    def yz_send(q):
        return far(own[1].at[q, 1 - y, z], ryz.at[q], s_yz.at[q], r_yz.at[q], across)

    def yz(k, q):
        b = (q, 1 - y, z)
        own[1][b] = (f(own[1][b]) + f(oth[1][b]) + f(rr[1][b]) + f(ll[1][b])).astype(BF)
        yz_send(q).start()

    def small(i, k, put):
        layer, _, s = what(k)
        rows, cols = cut(i, s)
        e, t = k % NL, i // DOWN
        block = (layer, y, z, c, rows, cols)
        there = ((om if put else m)[i].at[layer, rows, cols], (ov if put else v)[i].at[layer, rows, cols], (ow if put else w)[i].at[block])
        here = (mbuf[t].at[e], vbuf[t].at[e], wbuf[t].at[k % NW])
        sems = s_st if put else s_ld
        return [near(b, r, sems.at[e, h]) if put else near(r, b, sems.at[e, h]) for h, (r, b) in enumerate(zip(there, here, strict=True))]

    def final(k, q):
        yz_send(q).wait_recv()

        def of(i):
            wait(small(i, k, False))
            mb, vb, wb = (b[i // DOWN] for b in (mbuf, vbuf, wbuf))
            for part, d0, n, s0, col in pieces(i):
                r = pl.ds(d0, n)
                gr = f(own[part][q, y, z, r]) + f(oth[part][q, y, z, r])
                gr += f(ry[q, z, r]) + f(rr[0][q, z, r]) + f(ll[0][q, z, r]) if part == 0 else f(rr[1][q, y, z, r]) + f(ll[1][q, y, z, r]) + f(ryz[q, r])
                gr = f(gr.astype(BF))
                b = (pl.ds(s0, n), pl.ds(col * LANES, LANES))
                bm, bw = (k % NL, *b), (k % NW, *b)
                mm = 0.9 * mb[bm] + 0.1 * gr
                vv = 0.95 * vb[bm] + 0.05 * gr * gr
                ww = f(wb[bw])
                mb[bm] = mm
                vb[bm] = vv
                wb[bw] = (ww - 0.02 * (mm * lax.rsqrt(vv + 1e-8) + 0.1 * ww)).astype(BF)
            run(small(i, k, True))

        each(what(k)[1], of)

    def move(e, i, k, q, zz):
        layer, _, s = what(k)
        part = e // 3
        along = e % 4
        lo, hi = (0, zz + 1) if e in (0, 4) else (zz, LINE) if e in (1, 5) else (0, LINE) if part == 0 else (zz, zz + 1)
        blocks = lo if hi - lo == 1 else pl.ds(lo, hi - lo)
        dst = ow[i].at[(layer, ALL if e > 3 else y, blocks, c, *cut(i, s, part))]
        src = dst
        if hi - lo == 1 and e < 4:
            (r, cc), (r0, c0) = SHAPE[i], FIRST[i]
            rows = (pl.ds(r0, r - r0) if part else pl.ds(0, r0)) if i == DOWN else pl.ds(0, r)
            cols = pl.ds(0, cc) if i == DOWN else pl.ds(c0, cc - c0) if part else pl.ds(0, c0)
            src = wbuf[i // DOWN].at[k % NW, rows, cols]
        to = (right, left)[along] if along < 2 else across
        return far(src, dst, s_ag.at[e, q], r_ag.at[e, q], to)

    def events(zz):
        side = LINE - 1
        turn = max(zz, side - zz)
        out = [(0, None, 3), (1, (3, zz), None), (turn, None, 2), (turn + 1, (2, zz), None)]
        for part in range(2):
            for t, back, e, more_ in ((zz, zz - 1, 0, zz < side), (side - zz, zz + 1, 1, zz > 0)):
                e += 4 * part
                out.insert(0, (t + part, (e, back) if 0 <= back < LINE else None, e if more_ else None))
        return out

    def spread(t, zz, k, q):
        todo = [(w_, e) for step, w_, e in events(zz) if step == t]
        if t == 1:
            wait(small(GATE, k, True))
        for w_, _ in todo:
            if w_:
                move(w_[0], GATE, k, q, w_[1]).wait_recv()
        sends = [e for _, e in todo if e is not None]
        if sends:
            each(what(k)[1], lambda i: run([move(e, i, k, q, zz) for e in sends]))

    def over(i, k, q):
        layer, _, s = what(k)
        b = ow[i].at[(layer, ALL, ALL, c, *cut(i, s))]
        return far(b, b, s_c.at[q], r_c.at[k % (2 * NS)], core)

    def hand(k, q):
        each(what(k)[1], lambda i: over(i, k, q).start())

    def finish(zz, k, q):
        over(GATE, k, q).wait()
        for _, _, e in events(zz):
            if e is not None:
                move(e, GATE, k, q, zz).wait_send()

    def sent(zz, k, q):
        for part in range(2):
            exchange(q, part).wait_send()
            for to_right in (True, False):
                lo, hi = span(zz, to_right)
                if lo < hi:
                    line(part, q, zz, to_right).wait_send()
        y_send(q).wait_send()
        yz_send(q).wait_send()

    def spreads(i, zz):
        for t in range(LINE + 1):
            stage(i, LINE + t, functools.partial(spread, t, zz))
        stage(i, NS - 2, functools.partial(sent, zz))
        stage(i, LAST - 1, functools.partial(finish, zz))

    def communicate(i):
        stage(i, 0, first)
        stage(i, 1, lambda k, q: y_send(q).wait_recv())
        chip(lambda zz: lines(i, zz))
        stage(i, LINE - 1, yz)
        stage(i, LINE - 2, lambda k, q: each(what(k)[1], lambda e: run(small(e, k, False))))
        stage(i, LINE, final)
        chip(lambda zz: spreads(i, zz))
        stage(i, 2 * LINE, hand)

    def wload(layer, j, x):
        return [near(nat[h].at[layer, :, at(j, FB)], wgu.at[x, :, pl.ds(FB * h, FB)], s_w.at[x, h]) for h in range(2)]

    def wdload(layer, j, x):
        return near(nat[DOWN].at[layer, at(j, FB)], wd.at[x], s_wd.at[x])

    def x_tile(t):
        return near(x.at[at(t, TT)], dgu.at[at(t, TT), pl.ds(0, D)], s_x.at[t])

    def h1_tile(t):
        return near(dgu.at[at(t, TT), pl.ds(0, D)], h1.at[at(t, TT)], s_h1.at[t])

    def dy_tile(t):
        return near(dy.at[at(t, TT)], dv.at[at(t, TT)], s_dy.at[t])

    def a0_load():
        return near(a0, av, s_a0)

    def a0_keep():
        return near(av, a0, s_a0)

    def keep(j):
        return near(dgu, dgu_all.at[j], s_dgu)

    def dl(u):
        return near(dgu_all.at[u % BLOCKS, at(u // BLOCKS, HALF)], dgu.at[at(u % 2, HALF)], s_dl.at[u % 2])

    def gl(s, put=False):
        e = s % 3
        here = [(t.at[at(s % TILES, TT), at(s // TILES, FB)], gt.at[e, h]) for h, t in enumerate((gate0, up0))]
        return [near(b, t, s_keep.at[e, h]) if put else near(t, b, s_gt.at[e, h]) for h, (t, b) in enumerate(here)]

    def h1_load():
        return near(h1, av, s_h)

    def g_out(layer, j, t):
        return near(gout.at[t], g_gu.at[layer, j, t], s_go.at[t])

    def _rms(b):
        wide = f(b)
        return (wide * lax.rsqrt(jnp.mean(wide * wide, -1, keepdims=True) + 1e-6)).astype(BF)

    def down(s):
        rows, j = at(s % TILES, TT), s // TILES
        acc[rows] = jnp.where(j == 0, 0.0, acc[rows]) + _dot(hid[at(s % 2, TT)], wd[j % 2], 1, 0)

    def close(t):
        rows = at(t, TT)
        new = (f(dgu[rows, :D]) + f(acc[rows].astype(BF))).astype(BF)
        dgu[rows, :D] = new
        av[rows] = _rms(new)
        h1_tile(t).start()

    STEPS = BLOCKS * TILES

    def forward(p, closing=()):
        j = p // 2
        k, s = j % 2, 2 * p

        @pl.when(p % 2 == 0)
        def _():
            wait(wload(0, j, k))
            wdload(0, j, k).wait()

        @pl.when(p % 2 == 1)
        def _():
            last = j == BLOCKS - 1
            layer, nxt = jnp.where(last, 1, 0), jnp.where(last, 0, j + 1)
            run(wload(layer, nxt, 1 - k))
            wdload(layer, nxt, 1 - k).start()

        pl.when(p == 2)(lambda: a0_keep().start())
        pl.when(s == STEPS - TILES)(lambda: a0_keep().wait())
        pl.when(p > 1)(lambda: wait(gl(s - 3, True)))
        pl.when(p > 0)(lambda: wait(gl(s - 2, True)))
        for e in range(2):
            n = s + e
            gu = _dot(av[at(n % TILES, TT)], wgu[k], 1, 0)
            down(jnp.where(n == 0, TILES - 1, n - 1))
            gate, up = gu[:, :FB], gu[:, FB:]
            gt[n % 3, 0] = gate
            gt[n % 3, 1] = up
            hid[at(n % 2, TT)] = (gate * jax.nn.sigmoid(gate) * up).astype(BF)
            if e in closing:
                close((n - 1) % TILES)
            run(gl(n, True))

    def gated(rows, gate, up, dh):
        s = jax.nn.sigmoid(gate)
        gs = gate * s
        dh = f(dh.astype(BF))
        hid[rows] = (gs * up).astype(BF)
        dgu[rows, FB:] = (dh * gs).astype(BF)
        dgu[rows, :FB] = (dh * up * (s + gs * (1 - s))).astype(BF)

    def gu_half(t, layer, j):
        out = _dot(av[:, at(t, TT)], dgu[...], 0, 0).astype(BF)
        many = FB // LANES
        r = SHAPE[GATE][0]
        for n in range(2 * many):
            part = out[:, LANES * n : LANES * (n + 1)].reshape(LINE, 2, MANY, r, LANES)
            for b in range(MANY):
                gout[t, n // many, b, :, :, pl.ds(n % many * r, r)] = part[:, :, b]
        g_out(layer, j, t).start()

    def where(i):
        top, low = i < DA, (i >= LOW) & (i < END)
        ii = jnp.where(top, i, i - LOW)
        return top, low, ii // 4, ii % 4, jnp.where(top, 1, 0)

    def before(i):
        top, low, j, r, layer = where(i)

        @pl.when((top | low) & (r == 3))
        def _():
            wait([g_out(layer, j, t) for t in range(2)])

        stage(i, LEAD, fetch)

    def compute(i):
        top, low, j, r, layer = where(i)
        x = jnp.where(top, j + 1, j) % 2

        pl.when(((i > 4) & (i <= DA + 1) & (i % 4 == 1)) | ((i > LOW + 4) & (i <= END + 1) & (i % 4 == (LOW + 1) % 4)))(lambda: near(dout, dout, s_do).wait())

        @pl.when(top & (r == 0))
        def _():
            wait(wload(1, j, x))
            wdload(1, j, x).wait()
            pl.when(j > 0)(lambda: keep(j - 1).wait())

            @pl.when(j < BLOCKS - 1)
            def _():
                run(wload(1, j + 1, 1 - x))
                wdload(1, j + 1, 1 - x).start()

        @pl.when(top & (r < 2))
        def _():
            @pl.when(j == 0)
            def _():
                for t in range(2):
                    wait((dy_tile(2 * r + t), h1_tile(2 * r + t)))

            def one(t):
                rows = at(t, TT)
                gu = _dot(av[rows], wgu[x], 1, 0)
                gated(rows, gu[:, :FB], gu[:, FB:], _dot(dv[rows], wd[x], 1, 1))

            one(2 * r)
            one(2 * r + 1)
            pl.when(r == 1)(lambda: keep(j).start())

        @pl.when(low & (r == 0))
        def _():
            wdload(0, j, x).wait()
            pl.when(j < BLOCKS - 1)(lambda: wdload(0, j + 1, 1 - x).start())

        @pl.when(low & (r < 2))
        def _():
            def one(t):
                s = TILES * j + t
                wait(gl(s))
                pl.when(s < BLOCKS * TILES - 2)(lambda: run(gl(s + 2)))
                rows = at(t, TT)
                gated(rows, gt[s % 3, 0], gt[s % 3, 1], _dot(dv[rows], wd[x], 1, 1))

            loop(3 * r, 3 + r, one)

        @pl.when(top & (r == 2))
        def _():
            gu_half(0, layer, j)
            gu_half(1, layer, j)

        @pl.when(low & ((r == 1) | (r == 2)))
        def _():
            pl.when(i == LOW + 1)(lambda: a0_load().wait())
            gu_half(r - 1, layer, j)

        @pl.when((top | low) & (r == 3))
        def _():
            out = _dot(hid[...], dv[...], 0, 0)
            pp, n = dout.shape[:2]
            for p in range(pp):
                dout[p] = out[n * p : n * (p + 1)].astype(BF)

            def send(p):
                o = pp * j + p
                near(dout.at[p], g_down.at[layer, o // 40, (o // 10) % LINE, (o // 5) % 2, o % 5], s_do).start()

            loop(0, pp, send)

        @pl.when(i == DA - 1)
        def _():
            keep(BLOCKS - 1).wait()
            run(wload(1, 0, 0))
            dl(0).start()
            h1_load().start()

        @pl.when((i >= DA) & (i < LOW))
        def _():
            u = i - DA
            j, x = u % BLOCKS, u % 2
            wait(wload(1, j, x))
            dl(u).wait()

            @pl.when(i < LOW - 1)
            def _():
                run(wload(1, (u + 1) % BLOCKS, 1 - x))
                dl(u + 1).start()

            half = u // BLOCKS
            sums = at(half, HALF)
            acc[sums] = jnp.where(j == 0, 0.0, acc[sums]) + _dot(dgu[at(x, HALF)], wgu[x], 1, 1)

            @pl.when((j == BLOCKS - 1) | (u == BLOCKS))
            def _():
                pl.when(u < BLOCKS)(lambda: h1_load().wait())

                def one(t):
                    there = at(t, 256)
                    wide, da = f(av[there]), acc[there]
                    scale = lax.rsqrt(jnp.mean(wide * wide, -1, keepdims=True) + 1e-6)
                    inner = jnp.mean(wide * da, -1, keepdims=True)
                    back = (scale * da - wide * (scale * scale * scale * inner)).astype(BF)
                    dv[there] = (f(dv[there]) + f(back)).astype(BF)

                lo = jnp.where(u < BLOCKS, 0, jnp.where(u == BLOCKS, 2, 4))
                loop(lo, lo + jnp.where(u > BLOCKS, 4, 2), one)
                pl.when(u > BLOCKS)(lambda: a0_load().start())

        @pl.when(i == LOW - 2)
        def _():
            wdload(0, 0, 0).start()
            run(gl(0))
            run(gl(1))

    x_tile(0).start()
    run(wload(0, 0, 0))
    wdload(0, 0, 0).start()
    run([x_tile(t) for t in range(1, TILES)] + [dy_tile(t) for t in range(TILES)])
    hid[...] = jnp.zeros_like(hid)

    def norm(t):
        x_tile(t).wait()
        av[at(t, TT)] = _rms(dgu[at(t, TT), :D])

    loop(0, TILES, norm)
    loop(0, STEPS // 2 - 2, forward)
    forward(STEPS // 2 - 2, (1,))
    forward(STEPS // 2 - 1, (0, 1))
    down(STEPS - 1)
    close(TILES - 1)
    for s in range(STEPS - 3, STEPS):
        wait(gl(s, True))
    pl.semaphore_wait(barrier, 2 + jnp.where(more, 1, 0) + jnp.where(less, 1, 0))

    def tick(i):
        before(i)
        compute(i)
        communicate(i - LEAD)

    loop(0, N + LAST + LEAD, tick)


def step_scratch():
    d = pltpu.SemaphoreType.DMA
    ry, rz = ROWS

    def vm(*shape, dtype=BF):
        return pltpu.VMEM(shape, dtype)

    sums = [vm(NS, 2, LINE, r, LANES) for _ in range(2) for r in (ry, rz)]
    lines = [vm(NS, *r, LANES) for _ in range(2) for r in ((LINE, ry), (2, LINE, rz))]
    small = [vm(n, *SHAPE[i], dtype=t) for n, t in ((NL, F32), (NL, F32), (NW, BF)) for i in (UP, DOWN)]
    ring, two, parts, six = d((NS,)), d((NS, 2)), d((2, NS)), d((6, NS))
    sems = [two, two, two, ring, ring, parts, parts, parts, parts, ring, ring, d((NL, 3)), d((NL, 3)), six, six, ring, d((2 * NS,))]
    work = [vm(T, D), vm(T, D), vm(2, D, 2 * FB), vm(2, FB, D), vm(T, FB), vm(T, 2 * FB), vm(2, 2, MANY, LINE, 2, ry + rz, LANES), vm(16, 40, D)]
    work += [vm(T, D, dtype=F32), vm(3, 2, TT, FB, dtype=F32)]
    work += [d((TILES,)), d((TILES,)), d((2, 2)), d((2,)), d, d((2,)), d, d((2,)), d((3, 2)), d, d, d((3, 2)), d((TILES,))]
    return [*sums, *lines, *small, vm(NS, LINE, ry, LANES), vm(NS, rz, LANES), *sems, *work]


def hbm(n):
    return [pl.BlockSpec(memory_space=pl.ANY)] * n


def step_of(x, dy, w, m, v):
    def blocks(t, *tail):
        return (t.shape[0], 2, LINE, 2, *(tail or (t.shape[1] // 16,)), t.shape[-1])

    like = jax.ShapeDtypeStruct
    views = [t.reshape(blocks(t)) for t in w]
    args = [x, dy, *w, *views, *m, *v]
    outs = [like(t.shape, BF) for t in views] + [like(t.shape, F32) for t in (*m, *v)]
    outs += [like((2, BLOCKS, 2, 2, MANY, LINE, 2, sum(ROWS), LANES), BF), like(blocks(w[DOWN], 5, 40), BF), like((BLOCKS, T, 2 * FB), BF)]
    outs += [like((T, F), F32)] * 2 + [like((T, D), BF)] * 2
    new = pl.pallas_call(
        step_kernel,
        out_shape=outs,
        in_specs=hbm(len(args)),
        out_specs=hbm(len(outs)),
        scratch_shapes=step_scratch(),
        compiler_params=pltpu.CompilerParams(collective_id=0, has_side_effects=True, vmem_limit_bytes=67043328),
    )(*args)
    old = (*w, *m, *v)
    return copied([n.reshape(t.shape) for n, t in zip(new, old)])


def copy_kernel(n, *refs):
    src, dst, tmp = refs[:n], refs[n : 2 * n], refs[2 * n : 3 * n]
    s_in, s_out = refs[3 * n :]
    cuts = [(k, l, at(b, t.shape[1] // 4)) for k, t in enumerate(src) for l in range(2) for b in range(4 if t.dtype == BF else 0)]
    cuts += [(k, l, ALL) for k, t in enumerate(src) for l in range(2) if t.dtype == F32]
    ins = [near(src[k].at[l, r], tmp[k].at[l, r], s_in.at[e]) for e, (k, l, r) in enumerate(cuts)]
    outs = [near(tmp[k].at[l, r], dst[k].at[l, r], s_out.at[e]) for e, (k, l, r) in enumerate(cuts)]
    run(ins)
    for i, o in zip(ins, outs, strict=True):
        i.wait()
        o.start()
    wait(outs)


def copied(arrays):
    n = len(arrays)
    many = sum(8 if t.dtype == BF else 2 for t in arrays)
    return pl.pallas_call(
        functools.partial(copy_kernel, n),
        out_shape=[jax.ShapeDtypeStruct(t.shape, t.dtype) for t in arrays],
        in_specs=hbm(n),
        out_specs=hbm(n),
        scratch_shapes=[pltpu.VMEM(t.shape, t.dtype) for t in arrays] + [pltpu.SemaphoreType.DMA((many,))] * 2,
        compiler_params=pltpu.CompilerParams(vmem_limit_bytes=67043328),
    )(*arrays)


def solution(mesh):
    def step(x, dy, *arrays):
        w, m, v = (arrays[i : i + 3] for i in (0, 3, 6))
        return tuple(step_of(x[0], dy[0], w, m, v))

    one, whole, rows = P(("rep", "dp")), P(), P(None, "dp")
    return jax.shard_map(
        step,
        mesh=mesh,
        in_specs=(one, one) + (whole,) * 3 + (rows,) * 6,
        out_specs=(P("rep"),) * 3 + (P("rep", "dp"),) * 6,
        check_vma=False,
    )
```
